8 devices in a mesh: rep: 2 (over y, z), dp: 4 (over x, core).
Axes of the slice: x: 2, y: 2, z: 1, core: 2. Of those that a mesh axis runs over, the one named last changes fastest.
Arguments:
- x: bfloat16 [8, 2048, 1152], P(('rep', 'dp')), parts along dimension 0
- dy: bfloat16 [8, 2048, 1152], P(('rep', 'dp')), parts along dimension 0
- w_gate: bfloat16 [2, 1152, 4608], replicated
- w_up: bfloat16 [2, 1152, 4608], replicated
- w_down: bfloat16 [2, 4608, 1152], replicated
- m_w_gate: float32 [2, 1152, 4608], P(None, 'dp')
- m_w_up: float32 [2, 1152, 4608], P(None, 'dp')
- m_w_down: float32 [2, 4608, 1152], P(None, 'dp')
- v_w_gate: float32 [2, 1152, 4608], P(None, 'dp')
- v_w_up: float32 [2, 1152, 4608], P(None, 'dp')
- v_w_down: float32 [2, 4608, 1152], P(None, 'dp')
Outputs:
- output 1: bfloat16 [4, 1152, 4608], P('rep'), parts along dimension 0
- output 2: bfloat16 [4, 1152, 4608], P('rep'), parts along dimension 0
- output 3: bfloat16 [4, 4608, 1152], P('rep'), parts along dimension 0
- output 4: float32 [4, 1152, 4608], P('rep', 'dp'), parts along dimension 0
- output 5: float32 [4, 1152, 4608], P('rep', 'dp'), parts along dimension 0
- output 6: float32 [4, 4608, 1152], P('rep', 'dp'), parts along dimension 0
- output 7: float32 [4, 1152, 4608], P('rep', 'dp'), parts along dimension 0
- output 8: float32 [4, 1152, 4608], P('rep', 'dp'), parts along dimension 0
- output 9: float32 [4, 4608, 1152], P('rep', 'dp'), parts along dimension 0
There are 2 independent parts. The reference program is written for one: setup_inputs(seed, part) draws one part's arguments, and reference() takes and returns one part's arrays. A program takes and returns all parts, laid end to end along the dimension named above; an argument that names none is the same for every part.
All inputs are finite; a program needn't handle non-finite values.
Results may differ from the reference program's by a relative error of at most 0.022.
Values are sent between devices in bfloat16 or wider.
A program may use at most 2 GiB of HBM per device.

```python
import jax
import jax.numpy as jnp
from jax import lax

SEQUENCES = 4
TOKENS = 2048
D = 1152
FF = 4608
LAYERS = 2
NAMES = ("w_gate", "w_up", "w_down")
SHAPES = {"w_gate": (LAYERS, D, FF), "w_up": (LAYERS, D, FF), "w_down": (LAYERS, FF, D)}


def bump(key, n, height):
    away = (jnp.arange(n, dtype=jnp.int32) - jax.random.randint(key, (), 0, n, jnp.int32)) % n
    return jnp.where(away < n // 8, height, 1.0)


def together(key, own, strength):
    shared = jax.random.normal(key, own.shape[1:], jnp.float32)
    return (own + strength * shared) * lax.rsqrt(1 + strength * strength)


def setup_inputs(seed: int = 0, part: int = 0) -> dict:
    kx, kdy, ka, kb, kz, kf, kh, kl, *keys = jax.random.split(jax.random.key(seed), 8 + 3 * len(NAMES))
    kx, kdy, ka, kb = (jax.random.fold_in(k, part) for k in (kx, kdy, ka, kb))
    kw, km, kv = (keys[i::3] for i in range(3))
    shape = (SEQUENCES, TOKENS, D)
    much_x, much_dy = jax.random.uniform(kz, (2,), jnp.float32, 0.0, 1.0)
    loud = 2.0 ** jax.random.uniform(jax.random.fold_in(kz, 1), (), jnp.float32, -1.0, 2.0)
    layers = 2.0 ** jax.random.uniform(kl, (LAYERS, 1, 1), jnp.float32, -1.0, 1.0)
    x = together(ka, jax.random.normal(kx, shape, jnp.float32), much_x) * bump(kf, D, 4.0)
    dy = together(kb, jax.random.normal(kdy, shape, jnp.float32), much_dy)
    drawn = {"x": x.astype(jnp.bfloat16), "dy": (loud * dy * (SEQUENCES * TOKENS) ** -0.5).astype(jnp.bfloat16)}
    for key, name in zip(kw, NAMES, strict=True):
        w = jax.random.normal(key, SHAPES[name], jnp.float32) * SHAPES[name][1] ** -0.5
        drawn[name] = (w * {"w_gate": 1.0, "w_up": bump(kh, FF, 4.0), "w_down": layers}[name]).astype(jnp.bfloat16)
    for key, name in zip(km, NAMES, strict=True):
        drawn[f"m_{name}"] = 0.1 * jax.random.normal(key, SHAPES[name], jnp.float32)
    for key, name in zip(kv, NAMES, strict=True):
        drawn[f"v_{name}"] = jax.random.uniform(key, SHAPES[name], jnp.float32, 0.005, 0.015)
    return drawn


def matmul(a, w):
    return jnp.dot(a, w, preferred_element_type=jnp.float32).astype(jnp.bfloat16)


def normed(h):
    wide = h.astype(jnp.float32)
    scale = lax.rsqrt(jnp.mean(wide**2, -1, keepdims=True) + 1e-6)
    return (wide * scale).astype(jnp.bfloat16)


def layer(h, w):
    a = normed(h)
    gate = jnp.dot(a, w["w_gate"], preferred_element_type=jnp.float32)
    up = jnp.dot(a, w["w_up"], preferred_element_type=jnp.float32)
    return h + matmul((jax.nn.silu(gate) * up).astype(jnp.bfloat16), w["w_down"])


def adamw(w, m, v, g):
    m = 0.9 * m + 0.1 * g
    v = 0.95 * v + 0.05 * g * g
    step = m * lax.rsqrt(v + 1e-8) + 0.1 * w
    return (w - 0.02 * step).astype(jnp.bfloat16), m, v


def clipped(gradients, sum_of_squares, count):
    factor = jnp.minimum(1.0, 0.5 * lax.rsqrt(sum_of_squares / count + 1e-30))
    return [g * factor for g in gradients]


def stack(weights, h):
    return lax.scan(lambda h, w: (layer(h, w), None), h, weights)[0]


def reference(x, dy, w_gate, w_up, w_down, m_w_gate, m_w_up, m_w_down, v_w_gate, v_w_up, v_w_down):
    weights = dict(zip(NAMES, (w_gate, w_up, w_down), strict=True))

    def take(so_far, sequence):
        h, by_y = sequence
        _, back = jax.vjp(lambda w: stack(w, h), weights)
        return jax.tree.map(lambda total, term: total + term.astype(jnp.float32), so_far, back(by_y)[0]), None

    none_yet = {name: jnp.zeros(w.shape, jnp.float32) for name, w in weights.items()}
    by_weights, _ = lax.scan(take, none_yet, (x, dy))
    gradients = [by_weights[name].astype(jnp.bfloat16).astype(jnp.float32) for name in NAMES]
    gradients = clipped(gradients, sum(jnp.sum(g * g) for g in gradients), sum(g.size for g in gradients))
    new = [
        adamw(w.astype(jnp.float32), m, v, g)
        for w, m, v, g in zip((w_gate, w_up, w_down), (m_w_gate, m_w_up, m_w_down), (v_w_gate, v_w_up, v_w_down), gradients, strict=True)
    ]
    return tuple(one[which] for which in range(3) for one in new)
```

```python
import functools

import jax
import jax.numpy as jnp
from jax import lax
from jax.experimental import pallas as pl
from jax.experimental.pallas import tpu as pltpu
from jax.sharding import PartitionSpec as P

F32, BF16 = jnp.float32, jnp.bfloat16
DEVICES = 4
LANES = 128
ANY = pl.BlockSpec(memory_space=pl.ANY)
VMEM_BYTES = 67_043_328


def dot(a, b, dims):
    return lax.dot_general(a, b, (dims, ((), ())), preferred_element_type=F32)


NN, NT, TT = ((1,), (0,)), ((1,), (1,)), ((0,), (1,))


def sigmoid(x):
    return 1.0 / (1.0 + jnp.exp(-x))


def loop(n, body):
    lax.fori_loop(0, n, lambda i, c: (body(i), c)[1], 0)


def grads_kernel(
    x, dy, wg, wu, wd,
    gg, gu, gd, factor, gate_s, up_s, a0t_s, ht_s, mate, own, far, cross,
    AT, DD, DT, ACC, GR, ACT, DG, DU, WD, OWNB, MATEB, FARB, SQ, SQS,
    wsem, iosem, d2d_send, d2d_recv, own_sem, far_sem, x_send, x_recv, fsem, sq_send, sq_recv,
):
    T, D = x.shape
    F = wg.shape[2]
    W = DEVICES * LANES
    NT_ = F // W
    H = T // 2
    R = D // DEVICES
    me = lax.axis_index("dp")
    chip, core = me // 2, me % 2
    mate_id, cross_id = {"dp": chip * 2 + 1 - core}, {"dp": (1 - chip) * 2 + core}
    lo, hi = pl.ds(0, H), pl.ds(H, H)

    barrier = pltpu.get_barrier_semaphore()
    for k in range(1, DEVICES):
        pl.semaphore_signal(barrier, inc=1, device_id={"dp": (me + k) % DEVICES}, device_id_type=pl.DeviceIdType.MESH)
    pl.semaphore_wait(barrier, DEVICES - 1)

    def columns(p, j):
        return pl.ds(pl.multiple_of(p * (F // DEVICES) + j * LANES, LANES), LANES)

    def weights(l, j, q, bufs):
        slot = q % 2
        copies = []
        for p in range(DEVICES):
            piece = pl.ds(p * LANES, LANES)
            if bufs is not None:
                copies.append(pltpu.make_async_copy(wg.at[l, :, columns(p, j)], bufs[0].at[slot, :, piece], wsem.at[slot, 0, p]))
                copies.append(pltpu.make_async_copy(wu.at[l, :, columns(p, j)], bufs[1].at[slot, :, piece], wsem.at[slot, 1, p]))
            copies.append(pltpu.make_async_copy(wd.at[l, columns(p, j), :], WD.at[slot, piece, :], wsem.at[slot, 2, p]))
        return copies

    def start(copies):
        for c in copies:
            c.start()

    def wait(copies):
        for c in copies:
            c.wait()

    def d2d(t, k):
        return pltpu.make_async_remote_copy(
            src_ref=GR.at[k, :, 1 - core], dst_ref=mate.at[t, k], send_sem=d2d_send.at[k], recv_sem=d2d_recv.at[t],
            device_id=mate_id, device_id_type=pl.DeviceIdType.MESH)

    def keep(t, k):
        return pltpu.make_async_copy(GR.at[k, :, core], own.at[t, k], own_sem.at[k])

    def across(t):
        return pltpu.make_async_remote_copy(
            src_ref=far.at[t], dst_ref=cross.at[t], send_sem=x_send.at[t], recv_sem=x_recv.at[t],
            device_id=cross_id, device_id_type=pl.DeviceIdType.MESH)

    def far_loads(t):
        return [
            pltpu.make_async_copy(own.at[t, :, 1 - chip], OWNB, far_sem.at[0]),
            pltpu.make_async_copy(mate.at[t, :, 1 - chip], MATEB, far_sem.at[1]),
        ]

    def far_store(t):
        return pltpu.make_async_copy(FARB, far.at[t], far_sem.at[2])

    def mate_arrived(t):
        pltpu.make_async_copy(mate.at[t], mate.at[t], d2d_recv.at[t]).wait()

    def comm1(t):
        mate_arrived(t)
        for k in range(3):
            keep(t, k).wait()
        start(far_loads(t))

    def comm2(t):
        wait(far_loads(t))

    def far_sum():
        for k in range(3):
            for r in range(0, R, 32):
                rows = slice(r, r + 32)
                FARB[k, rows, :] = (OWNB[k, rows, :].astype(F32) + MATEB[k, rows, :].astype(F32)).astype(BF16)

    def comm3(t):
        far_store(t).start()

    def comm4(t):
        far_store(t).wait()
        across(t).start()

    def sent(t):
        for k in range(3):
            d2d(t, k).wait_send()

    def put(t, k, rows, value):
        n = value.shape[0]
        value = value.astype(BF16)
        if k < 2:
            for i in range(n // R):
                o = rows // R + i
                GR[k, o // 2, o % 2] = value[i * R : (i + 1) * R]
        else:
            for i in range(n // R):
                for o in range(DEVICES):
                    GR[k, o // 2, o % 2, :, (rows // R + i) * LANES : (rows // R + i + 1) * LANES] = value[
                        i * R : (i + 1) * R, o * LANES : (o + 1) * LANES
                    ]

    def ship(t, k):
        d2d(t, k).start()
        keep(t, k).start()

    def product_back(g_ref, u_ref, d_ref, r0):
        step = 16
        for r in range(0, H, step):
            g, u = g_ref(r, step), u_ref(r, step)
            d = d_ref[r : r + step, :].astype(BF16).astype(F32)
            s = sigmoid(g)
            si = g * s
            ACT[r0 + r : r0 + r + step, :] = (si * u).astype(BF16)
            DU[r0 + r : r0 + r + step, :] = (d * si).astype(BF16)
            DG[r0 + r : r0 + r + step, :] = (d * u * (s + si * (1.0 - s))).astype(BF16)

    def scaled(wide):
        return lax.rsqrt(jnp.mean(wide * wide, axis=0, keepdims=True) + 1e-6)

    def first_half(A, WG, WU):
        load_x = pltpu.make_async_copy(x, DD, iosem.at[0])
        load_x.start()
        start(weights(0, 0, 0, (WG, WU)))
        load_x.wait()

        def norm_x(i):
            r = pl.ds(pl.multiple_of(i * LANES, LANES), LANES)
            wide = DD[r, :].astype(F32)
            scale = lax.rsqrt(jnp.mean(wide * wide, axis=1, keepdims=True) + 1e-6)
            a = (wide * scale).astype(BF16)
            A[r, :] = a
            AT[:, r] = a.T
            DT[:, r] = DD[r, :].T
            ACC[:, r] = jnp.zeros((D, LANES), F32)

        loop(T // LANES, norm_x)
        save_a0t = pltpu.make_async_copy(AT, a0t_s, iosem.at[0])
        save_a0t.start()
        load_dy = pltpu.make_async_copy(dy, DD, iosem.at[1])
        load_dy.start()

        def forward(G0, U0, G1, U1):
            S = ((G0, U0), (G1, U1))

            def stores(j, half):
                return [
                    pltpu.make_async_copy(ref, to.at[j, pl.ds(half * H, H), :], iosem.at[2 + 2 * half + n])
                    for n, (ref, to) in enumerate(zip(S[half], (gate_s, up_s)))
                ]

            def projections(half, slot):
                rows = lo if half == 0 else hi
                S[half][0][...] = dot(A[rows, :], WG[slot], NN)
                S[half][1][...] = dot(A[rows, :], WU[slot], NN)

            def product(half):
                g_ref, u_ref = S[half]
                for r in range(0, H, 16):
                    g = g_ref[r : r + 16, :]
                    ACT[half * H + r : half * H + r + 16, :] = (g * sigmoid(g) * u_ref[r : r + 16, :]).astype(BF16)

            def down(rows, slot):
                ACC[:, rows] += dot(WD[slot], ACT[rows, :], TT)

            def tile(j):
                slot = j % 2
                wait(weights(0, j, j, (WG, WU)))

                @pl.when(j < NT_ - 1)
                def _():
                    start(weights(0, j + 1, j + 1, (WG, WU)))

                @pl.when(j == NT_ - 1)
                def _():
                    start(weights(1, 0, NT_, (WG, WU)))

                @pl.when(j > 0)
                def _():
                    wait(stores(j - 1, 0) + stores(j - 1, 1))

                projections(0, slot)
                start(stores(j, 0))
                projections(1, slot)
                product(0)
                start(stores(j, 1))
                down(lo, slot)
                product(1)
                down(hi, slot)

            loop(NT_, tile)
            wait(stores(NT_ - 1, 0) + stores(NT_ - 1, 1))

        pl.run_scoped(forward, *[pltpu.VMEM((H, W), F32)] * 4)
        save_a0t.wait()
        load_dy.wait()

        def norm_h(i):
            r = pl.ds(pl.multiple_of(i * LANES, LANES), LANES)
            h = (DT[:, r].astype(F32) + ACC[:, r].astype(BF16).astype(F32)).astype(BF16)
            ACC[:, r] = jnp.zeros((D, LANES), F32)
            wide = h.astype(F32)
            a = (wide * scaled(wide)).astype(BF16)
            AT[:, r] = a
            A[r, :] = a.T
            DT[:, r] = h

        loop(T // LANES, norm_h)
        save_h = pltpu.make_async_copy(DT, ht_s, iosem.at[0])
        save_h.start()
        save_h.wait()

        def turn_dy(i):
            r = pl.ds(pl.multiple_of(i * LANES, LANES), LANES)
            DT[:, r] = DD[r, :].T

        loop(T // LANES, turn_dy)

        def layer1(G0, U0, D0, G1, U1, D1):
            S = ((G0, U0, D0), (G1, U1, D1))

            def projections(half, slot):
                rows = lo if half == 0 else hi
                S[half][0][...] = dot(A[rows, :], WG[slot], NN)
                S[half][1][...] = dot(A[rows, :], WU[slot], NN)
                S[half][2][...] = dot(DD[rows, :], WD[slot], NT)

            def back(half):
                g_ref, u_ref, d_ref = S[half]
                product_back(lambda r, n: g_ref[r : r + n, :], lambda r, n: u_ref[r : r + n, :], d_ref, half * H)

            def da(rows, slot):
                ACC[:, rows] += dot(WG[slot], DG[rows, :], NT)
                ACC[:, rows] += dot(WU[slot], DU[rows, :], NT)

            def tile(j):
                slot = (NT_ + j) % 2
                wait(weights(1, j, NT_ + j, (WG, WU)))

                @pl.when(j < NT_ - 1)
                def _():
                    start(weights(1, j + 1, NT_ + j + 1, (WG, WU)))

                @pl.when(j == NT_ - 1)
                def _():
                    start(weights(0, 0, 2 * NT_, None))

                projections(0, slot)
                pl.when(j > 0)(lambda: comm1(j - 1))
                projections(1, slot)
                back(0)
                pl.when(j > 0)(lambda: comm2(j - 1))
                da(lo, slot)
                back(1)
                far_sum()
                pl.when(j > 0)(lambda: comm3(j - 1))
                da(hi, slot)

                @pl.when(j > 0)
                def _():
                    comm4(j - 1)
                    sent(j - 1)

                for k, lhs, rhs in ((2, DT, ACT), (0, AT, DG), (1, AT, DU)):
                    for i in range(2):
                        put(j, k, i * (D // 2), dot(lhs[i * (D // 2) : (i + 1) * (D // 2), :], rhs[...], NN))
                    ship(j, k)

            loop(NT_, tile)

        pl.run_scoped(layer1, *[pltpu.VMEM((H, W), F32)] * 6)

    pl.run_scoped(first_half, pltpu.VMEM((T, D), BF16), pltpu.VMEM((2, D, W), BF16), pltpu.VMEM((2, D, W), BF16))

    load_a0t = pltpu.make_async_copy(a0t_s, AT, iosem.at[0])
    load_a0t.start()

    def norm_back(HT):
        load_h = pltpu.make_async_copy(ht_s, HT, iosem.at[1])
        load_h.start()
        load_h.wait()

        def part(i):
            r = pl.ds(pl.multiple_of(i * LANES, LANES), LANES)
            wide = HT[:, r].astype(F32)
            scale = scaled(wide)
            da = ACC[:, r].astype(BF16).astype(F32)
            along = jnp.mean(da * wide, axis=0, keepdims=True) * (scale * scale * scale)
            dwide = (da * scale - wide * along).astype(BF16).astype(F32)
            dh = (DT[:, r].astype(F32) + dwide).astype(BF16)
            DT[:, r] = dh
            DD[r, :] = dh.T

        loop(T // LANES, part)

    pl.run_scoped(norm_back, pltpu.VMEM((D, T), BF16))
    load_a0t.wait()

    def layer0(GB, UB, D0, D1):
        S = (D0, D1)

        def loads(j):
            return [
                pltpu.make_async_copy(gate_s.at[j], GB.at[j % 2], iosem.at[2 + j % 2]),
                pltpu.make_async_copy(up_s.at[j], UB.at[j % 2], iosem.at[4 + j % 2]),
            ]

        start(loads(0))

        def tile(j):
            t = NT_ + j
            slot = j % 2
            wait(weights(0, j, 2 * NT_ + j, None))

            @pl.when(j < NT_ - 1)
            def _():
                start(weights(0, j + 1, 2 * NT_ + j + 1, None))
                start(loads(j + 1))

            def back(half):
                product_back(
                    lambda r, n: GB[slot, half * H + r : half * H + r + n, :],
                    lambda r, n: UB[slot, half * H + r : half * H + r + n, :],
                    S[half],
                    half * H,
                )

            S[0][...] = dot(DD[lo, :], WD[slot], NT)
            wait(loads(j))
            comm1(t - 1)
            S[1][...] = dot(DD[hi, :], WD[slot], NT)
            back(0)
            comm2(t - 1)
            sent(t - 1)
            half_sum = pl.ds(0, W)
            ACC[:, half_sum] = dot(DT[:, lo], ACT[lo, :], NN)
            back(1)
            far_sum()
            comm3(t - 1)
            for i in range(2):
                rows = slice(i * (D // 2), (i + 1) * (D // 2))
                put(t, 2, i * (D // 2), ACC[rows, half_sum] + dot(DT[rows, hi], ACT[hi, :], NN))
            ship(t, 2)
            comm4(t - 1)
            for k, rhs in ((0, DG), (1, DU)):
                for i in range(2):
                    put(t, k, i * (D // 2), dot(AT[i * (D // 2) : (i + 1) * (D // 2), :], rhs[...], NN))
                ship(t, k)

        loop(NT_, tile)

    pl.run_scoped(layer0, pltpu.VMEM((2, T, W), F32), pltpu.VMEM((2, T, W), F32), pltpu.VMEM((H, W), F32), pltpu.VMEM((H, W), F32))

    last = 2 * NT_ - 1
    comm1(last)
    comm2(last)
    far_sum()
    comm3(last)
    comm4(last)
    sent(last)

    def finish(GN, UN, DN, CB):
        SQ[...] = jnp.zeros_like(SQ)

        def outs(t):
            l, j = 1 - t // NT_, t % NT_
            copies = []
            for p in range(DEVICES):
                copies.append(pltpu.make_async_copy(GN.at[:, pl.ds(p * LANES, LANES)], gg.at[l, :, columns(p, j)], fsem.at[3 + p]))
                copies.append(pltpu.make_async_copy(UN.at[:, pl.ds(p * LANES, LANES)], gu.at[l, :, columns(p, j)], fsem.at[7 + p]))
            rows = pl.ds(pl.multiple_of(j * LANES, LANES), LANES)
            copies.append(pltpu.make_async_copy(DN, gd.at[l, rows, :], fsem.at[11]))
            return copies

        def one(t):
            across(t).wait()
            ins = [
                pltpu.make_async_copy(own.at[t, :, chip], OWNB, fsem.at[0]),
                pltpu.make_async_copy(mate.at[t, :, chip], MATEB, fsem.at[1]),
                pltpu.make_async_copy(cross.at[t], CB, fsem.at[2]),
            ]
            start(ins)

            @pl.when(t > 0)
            def _():
                wait(outs(t - 1))

            wait(ins)
            for k in range(3):
                total = OWNB[k].astype(F32) + MATEB[k].astype(F32) + CB[k].astype(F32)
                g = total.astype(BF16)
                wide = g.astype(F32)
                SQ[...] += jnp.sum((wide * wide).reshape(R // 8, 8, W), axis=0)
                if k == 0:
                    GN[...] = g
                elif k == 1:
                    UN[...] = g
                else:
                    tall = jnp.concatenate([g[:, q * LANES : (q + 1) * LANES] for q in range(DEVICES)], axis=0)
                    DN[...] = tall.T
            start(outs(t))

        loop(2 * NT_, one)
        wait(outs(last))

    pl.run_scoped(finish, pltpu.VMEM((R, W), BF16), pltpu.VMEM((R, W), BF16), pltpu.VMEM((LANES, D), BF16), pltpu.VMEM((3, R, W), BF16))

    mine = jnp.sum(SQ[...], keepdims=True)
    SQS[DEVICES] = jnp.broadcast_to(mine, (8, LANES))
    copies = [
        pltpu.make_async_remote_copy(
            src_ref=SQS.at[DEVICES], dst_ref=SQS.at[me], send_sem=sq_send.at[k - 1], recv_sem=sq_recv.at[k - 1],
            device_id={"dp": (me + k) % DEVICES}, device_id_type=pl.DeviceIdType.MESH)
        for k in range(1, DEVICES)
    ]
    start(copies)
    SQS[me] = jnp.broadcast_to(mine, (8, LANES))
    for k in range(1, DEVICES):
        pltpu.make_async_copy(SQS.at[(me + DEVICES - k) % DEVICES], SQS.at[(me + DEVICES - k) % DEVICES], sq_recv.at[k - 1]).wait()
        copies[k - 1].wait_send()
    total = (SQS[0] + SQS[1]) + (SQS[2] + SQS[3])
    count = 2.0 * 3.0 * D * F
    factor[...] = jnp.minimum(1.0, 0.5 * lax.rsqrt(total / count + 1e-30))


def gradients(x, dy, wg, wu, wd):
    T, D = x.shape
    F = wg.shape[2]
    W = DEVICES * LANES
    n, R = F // W, D // DEVICES
    tiles = 2 * n
    hbm = lambda *s, d=BF16: jax.ShapeDtypeStruct(s, d)
    outs = [
        hbm(2, R, F), hbm(2, R, F), hbm(2, F // DEVICES, D), hbm(8, LANES, d=F32),
        hbm(n, T, W, d=F32), hbm(n, T, W, d=F32), hbm(D, T), hbm(D, T),
        hbm(tiles, 3, 2, R, W), hbm(tiles, 3, 2, R, W), hbm(tiles, 3, R, W), hbm(tiles, 3, R, W),
    ]
    sem = pltpu.SemaphoreType.DMA
    return pl.pallas_call(
        grads_kernel,
        out_shape=outs,
        in_specs=[ANY] * 5,
        out_specs=[ANY] * 3 + [pl.BlockSpec(memory_space=pltpu.VMEM)] + [ANY] * 8,
        scratch_shapes=[
            pltpu.VMEM((D, T), BF16), pltpu.VMEM((T, D), BF16), pltpu.VMEM((D, T), BF16), pltpu.VMEM((D, T), F32),
            pltpu.VMEM((3, 2, 2, R, W), BF16),
            pltpu.VMEM((T, W), BF16), pltpu.VMEM((T, W), BF16), pltpu.VMEM((T, W), BF16), pltpu.VMEM((2, W, D), BF16),
            pltpu.VMEM((3, R, W), BF16), pltpu.VMEM((3, R, W), BF16), pltpu.VMEM((3, R, W), BF16),
            pltpu.VMEM((8, W), F32), pltpu.VMEM((DEVICES + 1, 8, LANES), F32),
            sem((2, 3, DEVICES)), sem((6,)), sem((3,)), sem((tiles,)), sem((3,)), sem((3,)),
            sem((tiles,)), sem((tiles,)), sem((12,)), sem((DEVICES - 1,)), sem((DEVICES - 1,)),
        ],
        compiler_params=pltpu.CompilerParams(collective_id=0, has_side_effects=True, vmem_limit_bytes=VMEM_BYTES),
        name="gradients",
    )(x, dy, wg, wu, wd)[:4]


def adamw(w, m, v, g):
    m = 0.9 * m + 0.1 * g
    v = 0.95 * v + 0.05 * g * g
    step = m * lax.rsqrt(v + 1e-8) + 0.1 * w
    return (w - 0.02 * step).astype(BF16), m, v


def other_chip(a):
    return lax.ppermute(a, "dp", [(i, i ^ 2) for i in range(4)])


def other_core(a):
    return lax.ppermute(a, "dp", [(i, i ^ 1) for i in range(4)])


def solution(mesh):
    def step(x, dy, *arrays):
        weights, m, v = (arrays[i : i + 3] for i in (0, 3, 6))
        me = lax.axis_index("dp")
        *g, factor = gradients(x[0], dy[0], *weights)
        factor = factor[0, 0]
        new = []
        for w, mm, vv, gg in zip(weights, m, v, g):
            rows = w.shape[1] // 4
            mine = lax.dynamic_slice(w, (0, me * rows, 0), (2, rows, w.shape[2])).astype(F32)
            new.append(adamw(mine, mm, vv, gg.astype(F32) * factor))
        whole = []
        for t, _, _ in new:
            rows = t.shape[1]
            far = other_chip(t)
            both = jnp.stack([t, far])
            mate = other_core(both)
            out = jnp.zeros((2, 4 * rows, t.shape[2]), BF16)
            for which, piece in ((me, t), (me ^ 2, far), (me ^ 1, mate[0]), (me ^ 3, mate[1])):
                out = lax.dynamic_update_slice(out, piece, (0, which * rows, 0))
            whole.append(out)
        return (*whole, *(n[1] for n in new), *(n[2] for n in new))

    rows = P(None, "dp", None)
    return jax.shard_map(
        step,
        mesh=mesh,
        in_specs=(P(("rep", "dp")), P(("rep", "dp")), *(P(),) * 3, *(rows,) * 6),
        out_specs=(*(P("rep"),) * 3, *(P("rep", "dp"),) * 6),
        check_vma=False,
    )
```

```python
import functools

import jax
import jax.numpy as jnp
from jax import lax
from jax.experimental import pallas as pl
from jax.experimental.pallas import tpu as pltpu
from jax.sharding import PartitionSpec as P


F32, BF16 = jnp.float32, jnp.bfloat16
DEVICES = 4
LANES = 128
ANY = pl.BlockSpec(memory_space=pl.ANY)
VMEM_BYTES = 67_043_328


def dot(a, b, dims):
    return lax.dot_general(a, b, (dims, ((), ())), preferred_element_type=F32)


NN, NT, TT = ((1,), (0,)), ((1,), (1,)), ((0,), (1,))


def sigmoid(x):
    return 1.0 / (1.0 + jnp.exp(-x))


def loop(n, body):
    lax.fori_loop(0, n, lambda i, c: (body(i), c)[1], 0)


def grads_kernel(
    x, dy, wg, wu, wd,
    gg, gu, gd, factor, gate_s, up_s, a0t_s, ht_s, mate, own, far, cross,
    AT, DD, DT, ACC, GR, ACT, DG, DU, WD, OWNB, MATEB, FARB, SQ, SQS,
    wsem, iosem, d2d_send, d2d_recv, own_sem, far_sem, x_send, x_recv, fsem, sq_send, sq_recv,
):
    T, D = x.shape
    F = wg.shape[2]
    W = DEVICES * LANES
    NT_ = F // W
    H = T // 2
    R = D // DEVICES
    me = lax.axis_index("dp")
    chip, core = me // 2, me % 2
    mate_id, cross_id = {"dp": chip * 2 + 1 - core}, {"dp": (1 - chip) * 2 + core}
    lo, hi = pl.ds(0, H), pl.ds(H, H)

    barrier = pltpu.get_barrier_semaphore()
    for k in range(1, DEVICES):
        pl.semaphore_signal(barrier, inc=1, device_id={"dp": (me + k) % DEVICES}, device_id_type=pl.DeviceIdType.MESH)
    pl.semaphore_wait(barrier, DEVICES - 1)

    def columns(p, j):
        return pl.ds(pl.multiple_of(p * (F // DEVICES) + j * LANES, LANES), LANES)

    def weights(l, j, q, bufs):
        slot = q % 2
        copies = []
        for p in range(DEVICES):
            piece = pl.ds(p * LANES, LANES)
            if bufs is not None:
                copies.append(pltpu.make_async_copy(wg.at[l, :, columns(p, j)], bufs[0].at[slot, :, piece], wsem.at[slot, 0, p]))
                copies.append(pltpu.make_async_copy(wu.at[l, :, columns(p, j)], bufs[1].at[slot, :, piece], wsem.at[slot, 1, p]))
            copies.append(pltpu.make_async_copy(wd.at[l, columns(p, j), :], WD.at[slot, piece, :], wsem.at[slot, 2, p]))
        return copies

    def start(copies):
        for c in copies:
            c.start()

    def wait(copies):
        for c in copies:
            c.wait()

    def d2d(t, k):
        return pltpu.make_async_remote_copy(
            src_ref=GR.at[k, :, 1 - core], dst_ref=mate.at[t, k], send_sem=d2d_send.at[k], recv_sem=d2d_recv.at[t],
            device_id=mate_id, device_id_type=pl.DeviceIdType.MESH)

    def keep(t, k):
        return pltpu.make_async_copy(GR.at[k, :, core], own.at[t, k], own_sem.at[k])

    def across(t):
        return pltpu.make_async_remote_copy(
            src_ref=far.at[t], dst_ref=cross.at[t], send_sem=x_send.at[t], recv_sem=x_recv.at[t],
            device_id=cross_id, device_id_type=pl.DeviceIdType.MESH)

    def far_loads(t):
        return [
            pltpu.make_async_copy(own.at[t, :, 1 - chip], OWNB, far_sem.at[0]),
            pltpu.make_async_copy(mate.at[t, :, 1 - chip], MATEB, far_sem.at[1]),
        ]

    def far_store(t):
        return pltpu.make_async_copy(FARB, far.at[t], far_sem.at[2])

    def mate_arrived(t):
        pltpu.make_async_copy(mate.at[t], mate.at[t], d2d_recv.at[t]).wait()

    def comm1(t):
        mate_arrived(t)
        for k in range(3):
            keep(t, k).wait()
        start(far_loads(t))

    def comm2(t):
        wait(far_loads(t))

    def far_sum():
        for k in range(3):
            for r in range(0, R, 32):
                rows = slice(r, r + 32)
                FARB[k, rows, :] = (OWNB[k, rows, :].astype(F32) + MATEB[k, rows, :].astype(F32)).astype(BF16)

    def comm3(t):
        far_store(t).start()

    def comm4(t):
        far_store(t).wait()
        across(t).start()

    def sent(t):
        for k in range(3):
            d2d(t, k).wait_send()

    def put(k, rows, value):
        n = value.shape[0]
        value = value.astype(BF16)
        if k < 2:
            for i in range(n // R):
                o = rows // R + i
                GR[k, o // 2, o % 2] = value[i * R : (i + 1) * R]
        else:
            for i in range(n // R):
                for o in range(DEVICES):
                    GR[k, o // 2, o % 2, :, (rows // R + i) * LANES : (rows // R + i + 1) * LANES] = value[
                        i * R : (i + 1) * R, o * LANES : (o + 1) * LANES
                    ]

    def ship(t, k):
        d2d(t, k).start()
        keep(t, k).start()

    def product_back(g_ref, u_ref, d_ref, r0):
        step = 16
        for r in range(0, H, step):
            g, u = g_ref(r, step), u_ref(r, step)
            d = d_ref[r : r + step, :].astype(BF16).astype(F32)
            s = sigmoid(g)
            si = g * s
            ACT[r0 + r : r0 + r + step, :] = (si * u).astype(BF16)
            DU[r0 + r : r0 + r + step, :] = (d * si).astype(BF16)
            DG[r0 + r : r0 + r + step, :] = (d * u * (s + si * (1.0 - s))).astype(BF16)

    def scaled(wide):
        return lax.rsqrt(jnp.mean(wide * wide, axis=0, keepdims=True) + 1e-6)

    def first_half(A, WG, WU):
        load_x = pltpu.make_async_copy(x, DD, iosem.at[0])
        load_x.start()
        start(weights(0, 0, 0, (WG, WU)))
        load_x.wait()

        def norm_x(i):
            r = pl.ds(pl.multiple_of(i * LANES, LANES), LANES)
            wide = DD[r, :].astype(F32)
            scale = lax.rsqrt(jnp.mean(wide * wide, axis=1, keepdims=True) + 1e-6)
            a = (wide * scale).astype(BF16)
            A[r, :] = a
            AT[:, r] = a.T
            DT[:, r] = DD[r, :].T
            ACC[:, r] = jnp.zeros((D, LANES), F32)

        loop(T // LANES, norm_x)
        save_a0t = pltpu.make_async_copy(AT, a0t_s, iosem.at[0])
        save_a0t.start()
        load_dy = pltpu.make_async_copy(dy, DD, iosem.at[1])
        load_dy.start()

        def forward(G0, U0, G1, U1):
            S = ((G0, U0), (G1, U1))

            def stores(j, half):
                return [
                    pltpu.make_async_copy(ref, to.at[j, pl.ds(half * H, H), :], iosem.at[2 + 2 * half + n])
                    for n, (ref, to) in enumerate(zip(S[half], (gate_s, up_s)))
                ]

            def projections(half, slot):
                rows = lo if half == 0 else hi
                S[half][0][...] = dot(A[rows, :], WG[slot], NN)
                S[half][1][...] = dot(A[rows, :], WU[slot], NN)

            def product(half):
                g_ref, u_ref = S[half]
                for r in range(0, H, 16):
                    g = g_ref[r : r + 16, :]
                    ACT[half * H + r : half * H + r + 16, :] = (g * sigmoid(g) * u_ref[r : r + 16, :]).astype(BF16)

            def down(rows, slot):
                ACC[:, rows] += dot(WD[slot], ACT[rows, :], TT)

            def tile(j):
                slot = j % 2
                wait(weights(0, j, j, (WG, WU)))

                @pl.when(j < NT_ - 1)
                def _():
                    start(weights(0, j + 1, j + 1, (WG, WU)))

                @pl.when(j == NT_ - 1)
                def _():
                    start(weights(1, 0, NT_, (WG, WU)))

                @pl.when(j > 0)
                def _():
                    wait(stores(j - 1, 0) + stores(j - 1, 1))

                projections(0, slot)
                start(stores(j, 0))
                projections(1, slot)
                product(0)
                start(stores(j, 1))
                down(lo, slot)
                product(1)
                down(hi, slot)

            loop(NT_, tile)
            wait(stores(NT_ - 1, 0) + stores(NT_ - 1, 1))

        pl.run_scoped(forward, *[pltpu.VMEM((H, W), F32)] * 4)
        save_a0t.wait()
        load_dy.wait()

        def norm_h(i):
            r = pl.ds(pl.multiple_of(i * LANES, LANES), LANES)
            h = (DT[:, r].astype(F32) + ACC[:, r].astype(BF16).astype(F32)).astype(BF16)
            ACC[:, r] = jnp.zeros((D, LANES), F32)
            wide = h.astype(F32)
            a = (wide * scaled(wide)).astype(BF16)
            AT[:, r] = a
            A[r, :] = a.T
            DT[:, r] = h

        loop(T // LANES, norm_h)
        save_h = pltpu.make_async_copy(DT, ht_s, iosem.at[0])
        save_h.start()
        save_h.wait()

        def turn_dy(i):
            r = pl.ds(pl.multiple_of(i * LANES, LANES), LANES)
            DT[:, r] = DD[r, :].T

        loop(T // LANES, turn_dy)

        def layer1(G0, U0, D0, G1, U1, D1):
            S = ((G0, U0, D0), (G1, U1, D1))

            def projections(half, slot):
                rows = lo if half == 0 else hi
                S[half][0][...] = dot(A[rows, :], WG[slot], NN)
                S[half][1][...] = dot(A[rows, :], WU[slot], NN)
                S[half][2][...] = dot(DD[rows, :], WD[slot], NT)

            def back(half):
                g_ref, u_ref, d_ref = S[half]
                product_back(lambda r, n: g_ref[r : r + n, :], lambda r, n: u_ref[r : r + n, :], d_ref, half * H)

            def da(rows, slot):
                ACC[:, rows] += dot(WG[slot], DG[rows, :], NT)
                ACC[:, rows] += dot(WU[slot], DU[rows, :], NT)

            def tile(j):
                slot = (NT_ + j) % 2
                wait(weights(1, j, NT_ + j, (WG, WU)))

                @pl.when(j < NT_ - 1)
                def _():
                    start(weights(1, j + 1, NT_ + j + 1, (WG, WU)))

                @pl.when(j == NT_ - 1)
                def _():
                    start(weights(0, 0, 2 * NT_, None))

                projections(0, slot)
                pl.when(j > 0)(lambda: comm1(j - 1))
                projections(1, slot)
                back(0)
                pl.when(j > 0)(lambda: comm2(j - 1))
                da(lo, slot)
                back(1)
                far_sum()
                pl.when(j > 0)(lambda: comm3(j - 1))
                da(hi, slot)

                @pl.when(j > 0)
                def _():
                    comm4(j - 1)
                    sent(j - 1)

                for k, lhs, rhs in ((2, DT, ACT), (0, AT, DG), (1, AT, DU)):
                    for i in range(2):
                        put(k, i * (D // 2), dot(lhs[i * (D // 2) : (i + 1) * (D // 2), :], rhs[...], NN))
                    ship(j, k)

            loop(NT_, tile)

        pl.run_scoped(layer1, *[pltpu.VMEM((H, W), F32)] * 6)

    pl.run_scoped(first_half, pltpu.VMEM((T, D), BF16), pltpu.VMEM((2, D, W), BF16), pltpu.VMEM((2, D, W), BF16))

    load_a0t = pltpu.make_async_copy(a0t_s, AT, iosem.at[0])
    load_a0t.start()

    def norm_back(HT):
        load_h = pltpu.make_async_copy(ht_s, HT, iosem.at[1])
        load_h.start()
        load_h.wait()

        def part(i):
            r = pl.ds(pl.multiple_of(i * LANES, LANES), LANES)
            wide = HT[:, r].astype(F32)
            scale = scaled(wide)
            da = ACC[:, r].astype(BF16).astype(F32)
            along = jnp.mean(da * wide, axis=0, keepdims=True) * (scale * scale * scale)
            dwide = (da * scale - wide * along).astype(BF16).astype(F32)
            dh = (DT[:, r].astype(F32) + dwide).astype(BF16)
            DT[:, r] = dh
            DD[r, :] = dh.T

        loop(T // LANES, part)

    pl.run_scoped(norm_back, pltpu.VMEM((D, T), BF16))
    load_a0t.wait()

    def layer0(GB, UB, D0, D1):
        S = (D0, D1)

        def loads(j):
            return [
                pltpu.make_async_copy(gate_s.at[j], GB.at[j % 2], iosem.at[2 + j % 2]),
                pltpu.make_async_copy(up_s.at[j], UB.at[j % 2], iosem.at[4 + j % 2]),
            ]

        start(loads(0))

        def tile(j):
            t = NT_ + j
            slot = j % 2
            wait(weights(0, j, 2 * NT_ + j, None))

            @pl.when(j < NT_ - 1)
            def _():
                start(weights(0, j + 1, 2 * NT_ + j + 1, None))
                start(loads(j + 1))

            def back(half):
                product_back(
                    lambda r, n: GB[slot, half * H + r : half * H + r + n, :],
                    lambda r, n: UB[slot, half * H + r : half * H + r + n, :],
                    S[half],
                    half * H,
                )

            S[0][...] = dot(DD[lo, :], WD[slot], NT)
            wait(loads(j))
            comm1(t - 1)
            S[1][...] = dot(DD[hi, :], WD[slot], NT)
            back(0)
            comm2(t - 1)
            sent(t - 1)
            half_sum = pl.ds(0, W)
            ACC[:, half_sum] = dot(DT[:, lo], ACT[lo, :], NN)
            back(1)
            far_sum()
            comm3(t - 1)
            for i in range(2):
                rows = slice(i * (D // 2), (i + 1) * (D // 2))
                put(2, i * (D // 2), ACC[rows, half_sum] + dot(DT[rows, hi], ACT[hi, :], NN))
            ship(t, 2)
            comm4(t - 1)
            for k, rhs in ((0, DG), (1, DU)):
                for i in range(2):
                    put(k, i * (D // 2), dot(AT[i * (D // 2) : (i + 1) * (D // 2), :], rhs[...], NN))
                ship(t, k)

        loop(NT_, tile)

    pl.run_scoped(layer0, pltpu.VMEM((2, T, W), F32), pltpu.VMEM((2, T, W), F32), pltpu.VMEM((H, W), F32), pltpu.VMEM((H, W), F32))

    last = 2 * NT_ - 1
    comm1(last)
    comm2(last)
    far_sum()
    comm3(last)
    comm4(last)
    sent(last)

    def finish(GN, UN, DN, CB):
        SQ[...] = jnp.zeros_like(SQ)

        def outs(t):
            l, j = 1 - t // NT_, t % NT_
            copies = []
            for p in range(DEVICES):
                copies.append(pltpu.make_async_copy(GN.at[:, pl.ds(p * LANES, LANES)], gg.at[l, :, columns(p, j)], fsem.at[3 + p]))
                copies.append(pltpu.make_async_copy(UN.at[:, pl.ds(p * LANES, LANES)], gu.at[l, :, columns(p, j)], fsem.at[7 + p]))
            rows = pl.ds(pl.multiple_of(j * LANES, LANES), LANES)
            copies.append(pltpu.make_async_copy(DN, gd.at[l, rows, :], fsem.at[11]))
            return copies

        def one(t):
            across(t).wait()
            ins = [
                pltpu.make_async_copy(own.at[t, :, chip], OWNB, fsem.at[0]),
                pltpu.make_async_copy(mate.at[t, :, chip], MATEB, fsem.at[1]),
                pltpu.make_async_copy(cross.at[t], CB, fsem.at[2]),
            ]
            start(ins)

            @pl.when(t > 0)
            def _():
                wait(outs(t - 1))

            wait(ins)
            for k in range(3):
                total = OWNB[k].astype(F32) + MATEB[k].astype(F32) + CB[k].astype(F32)
                g = total.astype(BF16)
                wide = g.astype(F32)
                SQ[...] += jnp.sum((wide * wide).reshape(R // 8, 8, W), axis=0)
                if k == 0:
                    GN[...] = g
                elif k == 1:
                    UN[...] = g
                else:
                    tall = jnp.concatenate([g[:, q * LANES : (q + 1) * LANES] for q in range(DEVICES)], axis=0)
                    DN[...] = tall.T
            start(outs(t))

        loop(2 * NT_, one)
        wait(outs(last))

    pl.run_scoped(finish, pltpu.VMEM((R, W), BF16), pltpu.VMEM((R, W), BF16), pltpu.VMEM((LANES, D), BF16), pltpu.VMEM((3, R, W), BF16))

    mine = jnp.sum(SQ[...], keepdims=True)
    SQS[DEVICES] = jnp.broadcast_to(mine, (8, LANES))
    copies = [
        pltpu.make_async_remote_copy(
            src_ref=SQS.at[DEVICES], dst_ref=SQS.at[me], send_sem=sq_send.at[k - 1], recv_sem=sq_recv.at[k - 1],
            device_id={"dp": (me + k) % DEVICES}, device_id_type=pl.DeviceIdType.MESH)
        for k in range(1, DEVICES)
    ]
    start(copies)
    SQS[me] = jnp.broadcast_to(mine, (8, LANES))
    for k in range(1, DEVICES):
        pltpu.make_async_copy(SQS.at[(me + DEVICES - k) % DEVICES], SQS.at[(me + DEVICES - k) % DEVICES], sq_recv.at[k - 1]).wait()
        copies[k - 1].wait_send()
    total = (SQS[0] + SQS[1]) + (SQS[2] + SQS[3])
    count = 2.0 * 3.0 * D * F
    factor[...] = jnp.minimum(1.0, 0.5 * lax.rsqrt(total / count + 1e-30))


def gradients(x, dy, wg, wu, wd):
    T, D = x.shape
    F = wg.shape[2]
    W = DEVICES * LANES
    n, R = F // W, D // DEVICES
    tiles = 2 * n
    hbm = lambda *s, d=BF16: jax.ShapeDtypeStruct(s, d)
    outs = [
        hbm(2, R, F), hbm(2, R, F), hbm(2, F // DEVICES, D), hbm(8, LANES, d=F32),
        hbm(n, T, W, d=F32), hbm(n, T, W, d=F32), hbm(D, T), hbm(D, T),
        hbm(tiles, 3, 2, R, W), hbm(tiles, 3, 2, R, W), hbm(tiles, 3, R, W), hbm(tiles, 3, R, W),
    ]
    sem = pltpu.SemaphoreType.DMA
    return pl.pallas_call(
        grads_kernel,
        out_shape=outs,
        in_specs=[ANY] * 5,
        out_specs=[ANY] * 3 + [pl.BlockSpec(memory_space=pltpu.VMEM)] + [ANY] * 8,
        scratch_shapes=[
            pltpu.VMEM((D, T), BF16), pltpu.VMEM((T, D), BF16), pltpu.VMEM((D, T), BF16), pltpu.VMEM((D, T), F32),
            pltpu.VMEM((3, 2, 2, R, W), BF16),
            pltpu.VMEM((T, W), BF16), pltpu.VMEM((T, W), BF16), pltpu.VMEM((T, W), BF16), pltpu.VMEM((2, W, D), BF16),
            pltpu.VMEM((3, R, W), BF16), pltpu.VMEM((3, R, W), BF16), pltpu.VMEM((3, R, W), BF16),
            pltpu.VMEM((8, W), F32), pltpu.VMEM((DEVICES + 1, 8, LANES), F32),
            sem((2, 3, DEVICES)), sem((6,)), sem((3,)), sem((tiles,)), sem((3,)), sem((3,)),
            sem((tiles,)), sem((tiles,)), sem((12,)), sem((DEVICES - 1,)), sem((DEVICES - 1,)),
        ],
        compiler_params=pltpu.CompilerParams(collective_id=0, has_side_effects=True, vmem_limit_bytes=VMEM_BYTES),
        name="gradients",
    )(x, dy, wg, wu, wd)[:4]


def adamw_kernel(me, factor, g, w, m, v, *refs):
    out, send, new_m, new_v, turn = refs[-5:]
    turn[0] = me[0]
    grad = g[...].astype(F32) * factor[0:1, 0:1]
    one = 0.9 * m[...] + 0.1 * grad
    two = 0.95 * v[...] + 0.05 * grad * grad
    wide = w[...].astype(F32)
    new_w = (wide - 0.02 * (one * lax.rsqrt(two + 1e-8) + 0.1 * wide)).astype(BF16)
    out[...] = new_w
    send[...] = new_w
    new_m[...] = one
    new_v[...] = two


def adamw(me, factor, g, w, m, v, so_far, layer, first, steps, by_columns):
    rows = m.shape[1] if by_columns else LANES
    cols = DEVICES * LANES if by_columns else m.shape[2]
    tile = (None, rows, cols)
    if by_columns:
        block = pl.BlockSpec(tile, lambda i, me: (layer, 0, first + i))
        whole = pl.BlockSpec(tile, lambda i, me: (layer, me[0], first + i))
        alone, send = (rows, steps * cols), pl.BlockSpec((rows, cols), lambda i, me: (0, i))
    else:
        n = m.shape[1] // LANES
        block = pl.BlockSpec(tile, lambda i, me: (layer, first + i, 0))
        whole = pl.BlockSpec(tile, lambda i, me: (layer, me[0] * n + first + i, 0))
        alone, send = (steps * rows, cols), pl.BlockSpec((rows, cols), lambda i, me: (i, 0))
    begun = so_far is not None
    shape = lambda a: jax.ShapeDtypeStruct(a.shape, a.dtype)
    out, sent, new_m, new_v, turn = pl.pallas_call(
        adamw_kernel,
        grid_spec=pltpu.PrefetchScalarGridSpec(
            num_scalar_prefetch=1,
            grid=(steps,),
            in_specs=[pl.BlockSpec((8, LANES), lambda i, me: (0, 0)), block, whole, block, block] + [ANY] * (3 * begun),
            out_specs=[whole, send, block, block, pl.BlockSpec(memory_space=pltpu.SMEM)],
        ),
        out_shape=[shape(w), jax.ShapeDtypeStruct(alone, BF16), shape(m), shape(v), shape(me)],
        input_output_aliases={6: 0, 7: 2, 8: 3} if begun else {},
        compiler_params=pltpu.CompilerParams(vmem_limit_bytes=VMEM_BYTES),
        cost_estimate=pl.CostEstimate(flops=20 * steps * rows * cols, bytes_accessed=28 * steps * rows * cols, transcendentals=0),
        name="adamw",
    )(me, factor, g, w, m, v, *(so_far or ()))
    return (out, new_m, new_v), sent, turn


def place_kernel(n, at, me_ref, _, *refs):
    pieces, out, turn, bufs, sems = refs[:n], refs[n], refs[n + 1], refs[n + 2 : 2 * n + 2], refs[2 * n + 2]
    turn[0] = me_ref[0]
    loads = [pltpu.make_async_copy(p, b, sems.at[0, k]) for k, (p, b) in enumerate(zip(pieces, bufs))]
    for c in loads:
        c.start()
    stores = []
    for k in range(n):
        loads[k].wait()
        stores.append(pltpu.make_async_copy(bufs[k], out.at[at(k, me_ref[0])], sems.at[1, k]))
        stores[k].start()
    for c in stores:
        c.wait()


def place(out, me, pieces, owners, layer, first, by_columns):
    rows, cols = pieces[0].shape

    def at(k, me):
        owner = me ^ owners[k]
        if by_columns:
            return layer, pl.ds(pl.multiple_of(owner * rows, 8), rows), pl.ds(first * DEVICES * LANES, cols)
        return layer, pl.ds(pl.multiple_of(owner * (out.shape[1] // DEVICES) + first * LANES, LANES), rows), slice(None)

    n = len(pieces)
    return pl.pallas_call(
        functools.partial(place_kernel, n, at),
        in_specs=[pl.BlockSpec(memory_space=pltpu.SMEM)] + [ANY] * (n + 1),
        out_specs=[ANY, pl.BlockSpec(memory_space=pltpu.SMEM)],
        out_shape=[jax.ShapeDtypeStruct(out.shape, out.dtype), jax.ShapeDtypeStruct(me.shape, me.dtype)],
        scratch_shapes=[pltpu.VMEM((rows, cols), BF16)] * n + [pltpu.SemaphoreType.DMA((2, n))],
        input_output_aliases={1: 0},
        compiler_params=pltpu.CompilerParams(vmem_limit_bytes=VMEM_BYTES),
        cost_estimate=pl.CostEstimate(flops=4 * n * rows * cols, bytes_accessed=4 * n * rows * cols, transcendentals=0),
        name="place",
    )(me, out, *pieces)


def other_chip(a):
    return lax.ppermute(a, "dp", [(i, i ^ 2) for i in range(4)])


def other_core(a):
    return lax.ppermute(a, "dp", [(i, i ^ 1) for i in range(4)])


CHUNKS = (
    (0, 0, 0, 1), (0, 0, 1, 3), (0, 0, 4, 5), (0, 1, 0, 9), (1, 0, 0, 9), (1, 1, 0, 9), (2, 0, 0, 9), (2, 1, 0, 5), (2, 1, 5, 3), (2, 1, 8, 1),
)


def solution(mesh):
    def step(x, dy, *arrays):
        weights, m, v = (arrays[i : i + 3] for i in (0, 3, 6))
        me = lax.axis_index("dp").astype(jnp.int32).reshape(1)
        *g, factor = gradients(x[0], dy[0], *weights)
        new = [None] * 3
        gathered = []
        for k, layer, first, steps in CHUNKS:
            new[k], sent, me = adamw(me, factor, g[k], weights[k], m[k], v[k], new[k], layer, first, steps, k < 2)
            far = other_chip(sent)
            own = other_core(sent)
            gathered.append((far, own, other_core(far)))
        whole = [n[0] for n in new]
        for (k, layer, first, steps), pieces in zip(CHUNKS, gathered):
            whole[k], me = place(whole[k], me, pieces, (2, 1, 3), layer, first, k < 2)
        return (*whole, *(n[1] for n in new), *(n[2] for n in new))

    rows = P(None, "dp", None)
    return jax.shard_map(
        step,
        mesh=mesh,
        in_specs=(P(("rep", "dp")), P(("rep", "dp")), *(P(),) * 3, *(rows,) * 6),
        out_specs=(*(P("rep"),) * 3, *(P("rep", "dp"),) * 6),
        check_vma=False,
    )
```

```python
import functools

import jax
import jax.numpy as jnp
from jax import lax
from jax.experimental import pallas as pl
from jax.experimental.pallas import tpu as pltpu
from jax.sharding import PartitionSpec as P


F32, BF16 = jnp.float32, jnp.bfloat16
DEVICES = 4
LANES = 128
CHUNK = 256
ANY = pl.BlockSpec(memory_space=pl.ANY)
VMEM_BYTES = 67_043_328


def dot(a, b, dims):
    return lax.dot_general(a, b, (dims, ((), ())), preferred_element_type=F32)


NN, NT, TT = ((1,), (0,)), ((1,), (1,)), ((0,), (1,))


def sigmoid(x):
    return 1.0 / (1.0 + jnp.exp(-x))


def loop(n, body):
    lax.fori_loop(0, n, lambda i, c: (body(i), c)[1], 0)


def apart(cond, body):
    lax.fori_loop(0, jnp.where(cond, 1, 0), lambda i, c: (body(), c)[1], 0)


def grads_kernel(
    x, dy, wg, wu, wd,
    gg, gu, gd, factor, gate_s, up_s, a0t_s, ht_s, mate, own, far, cross,
    A, AT, DD, DT, ACC, GR, ACT, DG, DU, WG, WU, WD, G0, U0, D0, G1, U1, D1, MATEB, FB, SQ, SQS,
    wsem, iosem, d2d_send, d2d_recv, near_recv, free, own_sem, far_sem, x_send, x_recv, fsem, sq_send, sq_recv,
):
    T, D = x.shape
    F = wg.shape[2]
    W = DEVICES * LANES
    NT_ = F // W
    FAR, NEAR = 0, 1
    H = T // 2
    R = D // DEVICES
    me = lax.axis_index("dp")
    chip, core = me // 2, me % 2
    mate_id, cross_id = {"dp": chip * 2 + 1 - core}, {"dp": (1 - chip) * 2 + core}
    lo, hi = pl.ds(0, H), pl.ds(H, H)

    barrier = pltpu.get_barrier_semaphore()
    for k in range(1, DEVICES):
        pl.semaphore_signal(barrier, inc=1, device_id={"dp": (me + k) % DEVICES}, device_id_type=pl.DeviceIdType.MESH)

    def columns(p, j):
        return pl.ds(pl.multiple_of(p * (F // DEVICES) + j * LANES, LANES), LANES)

    def weights(l, j, q, down_only=False):
        slot = q % 2
        copies = []
        for p in range(DEVICES):
            piece = pl.ds(p * LANES, LANES)
            if not down_only:
                copies.append(pltpu.make_async_copy(wg.at[l, :, columns(p, j)], WG.at[slot, :, piece], wsem.at[slot, 0, p]))
                copies.append(pltpu.make_async_copy(wu.at[l, :, columns(p, j)], WU.at[slot, :, piece], wsem.at[slot, 1, p]))
            copies.append(pltpu.make_async_copy(wd.at[l, columns(p, j), :], WD.at[slot, piece, :], wsem.at[slot, 2, p]))
        return copies

    def start(copies):
        for c in copies:
            c.start()

    def wait(copies):
        for c in copies:
            c.wait()

    def owner_chip(side):
        return 1 - chip if side == FAR else chip

    def d2d(t, side):
        return pltpu.make_async_remote_copy(
            src_ref=GR.at[:, owner_chip(side), 1 - core], dst_ref=MATEB if side == FAR else mate.at[t],
            send_sem=d2d_send.at[side], recv_sem=d2d_recv if side == FAR else near_recv.at[t],
            device_id=mate_id, device_id_type=pl.DeviceIdType.MESH)

    def keep(t):
        return pltpu.make_async_copy(GR.at[:, chip, core], own.at[t], own_sem)

    def across(t, direct):
        return pltpu.make_async_remote_copy(
            src_ref=FB.at[t % 2] if direct else far.at[t], dst_ref=cross.at[t], send_sem=x_send.at[t], recv_sem=x_recv.at[t],
            device_id=cross_id, device_id_type=pl.DeviceIdType.MESH)

    def far_store(t):
        return pltpu.make_async_copy(FB.at[t % 2], far.at[t], far_sem)

    def send_far(t):
        pl.when(t > 0)(lambda: pl.semaphore_wait(free, 1))
        d2d(t, FAR).start()

    def far_sum(t):
        d2d(t, FAR).wait_recv()

        def some(i):
            rows = pl.ds(pl.multiple_of(i * 96, 96), 96)
            for k in range(3):
                FB[t % 2, k, rows, :] = (GR[k, 1 - chip, core, rows, :].astype(F32) + MATEB[k, rows, :].astype(F32)).astype(BF16)

        loop(R // 96, some)
        pl.semaphore_signal(free, inc=1, device_id=mate_id, device_id_type=pl.DeviceIdType.MESH)

    def sent(t):
        d2d(t, FAR).wait_send()
        d2d(t, NEAR).wait_send()
        keep(t).wait()

    def put(k, h, value, first=0):
        value = value.astype(BF16)
        for o in range(2):
            if k < 2:
                GR[k, h, o] = value[o * R : (o + 1) * R]
            else:
                for q in range(value.shape[0] // R):
                    lanes = slice((first + q) * LANES, (first + q + 1) * LANES)
                    GR[k, h, o, :, lanes] = value[q * R : (q + 1) * R, o * LANES : (o + 1) * LANES]

    def side_of(i):
        return jnp.where(i == 0, 1 - chip, chip)

    def hidden_of(h):
        return pl.ds(pl.multiple_of(h * (W // 2), W // 2), W // 2)

    def half_of(i):
        return pl.ds(pl.multiple_of(i * (D // 2), D // 2), D // 2)

    def product_back(g_ref, u_ref, d_ref, r0):
        step = 16
        for r in range(0, H, step):
            g, u = g_ref(r, step), u_ref(r, step)
            d = d_ref[r : r + step, :].astype(F32)
            s = sigmoid(g)
            si = g * s
            ACT[r0 + r : r0 + r + step, :] = (si * u).astype(BF16)
            DU[r0 + r : r0 + r + step, :] = (d * si).astype(BF16)
            DG[r0 + r : r0 + r + step, :] = (d * u * (s + si * (1.0 - s))).astype(BF16)

    def columns_of(i):
        return pl.ds(pl.multiple_of(i * CHUNK, CHUNK), CHUNK)

    def down_rows(step, body):
        for r in range(0, D, step):
            body(slice(r, r + step))

    def folded(t):
        return jnp.sum(t.reshape(t.shape[0] // 8, 8, t.shape[1]), axis=0)

    def turn(src, rows, dst):
        for c in range(0, T, 2 * LANES):
            dst[rows, c : c + 2 * LANES] = src[c : c + 2 * LANES, rows].T

    def loads(j):
        return [
            pltpu.make_async_copy(to.at[j, pl.ds(half * H, H), :], ref, iosem.at[3 + 2 * half + n])
            for half, refs in enumerate(((G0, U0), (G1, U1)))
            for n, (ref, to) in enumerate(zip(refs, (gate_s, up_s)))
        ]

    def load_h(HB, i):
        return pltpu.make_async_copy(ht_s.at[i], HB.at[i % 2], iosem.at[1 + i % 2])

    load_a0t = pltpu.make_async_copy(a0t_s, AT, iosem.at[0])

    def norm_back(HB):
        n = T // CHUNK

        def part(i):
            r = columns_of(i)
            slot = i % 2
            load_h(HB, i).wait()

            squares, along = [], []

            def add(rows):
                wide = HB[slot, rows, :].astype(F32)
                squares.append(folded(wide * wide))
                along.append(folded(ACC[rows, r].astype(BF16).astype(F32) * wide))

            down_rows(64, add)
            scale = lax.rsqrt(jnp.sum(sum(squares), axis=0, keepdims=True) / D + 1e-6)
            shrink = jnp.sum(sum(along), axis=0, keepdims=True) / D * (scale * scale * scale)

            def back(rows):
                wide = HB[slot, rows, :].astype(F32)
                dwide = ACC[rows, r].astype(BF16).astype(F32) * scale - wide * shrink
                dh = (DT[rows, r].astype(F32) + dwide.astype(BF16).astype(F32)).astype(BF16)
                DT[rows, r] = dh
                DD[r, rows] = dh.T

            down_rows(LANES, back)
            apart(i < n - 2, lambda: load_h(HB, i + 2).start())

        loop(n, part)
        sent(NT_ - 1)
        load_a0t.start()

    def first_half():
        S = ((G0, U0, D0), (G1, U1, D1))

        def forward(TB):
            load_x = [pltpu.make_async_copy(x.at[pl.ds(c * (T // 4), T // 4)], DD.at[pl.ds(c * (T // 4), T // 4)], iosem.at[c]) for c in range(4)]
            start(load_x)
            start(weights(0, 0, 0))

            def zero(i):
                ACC[pl.ds(pl.multiple_of(i * LANES, LANES), LANES), :] = jnp.zeros((LANES, T), F32)

            loop(D // LANES, zero)

            def norm_x(i):
                r = pl.ds(pl.multiple_of(i * LANES, LANES), LANES)
                wide = DD[r, :].astype(F32)
                A[r, :] = (wide * lax.rsqrt(jnp.mean(wide * wide, axis=1, keepdims=True) + 1e-6)).astype(BF16)
                AT[:, r] = DD[r, :].T

            for c in range(4):
                load_x[c].wait()
                loop(T // 4 // LANES, lambda i, c=c: norm_x(c * (T // 4 // LANES) + i))
            load_dy = pltpu.make_async_copy(dy, DD, iosem.at[6])
            load_dy.start()

            def stores(j, half):
                return [
                    pltpu.make_async_copy(ref, to.at[j, pl.ds(half * H, H), :], iosem.at[2 * half + n])
                    for n, (ref, to) in enumerate(zip(S[half][:2], (gate_s, up_s)))
                ]

            def save(j):
                return pltpu.make_async_copy(TB.at[j % 2], a0t_s.at[pl.ds(pl.multiple_of(j * LANES, LANES), LANES), :], iosem.at[4 + j % 2])

            def projections(half, slot):
                rows = lo if half == 0 else hi
                S[half][0][...] = dot(A[rows, :], WG[slot], NN)
                S[half][1][...] = dot(A[rows, :], WU[slot], NN)

            def product(half):
                g_ref, u_ref, _ = S[half]
                for r in range(0, H, 16):
                    g = g_ref[r : r + 16, :]
                    ACT[half * H + r : half * H + r + 16, :] = (g * sigmoid(g) * u_ref[r : r + 16, :]).astype(BF16)

            def down(rows, slot):
                ACC[:, rows] += dot(WD[slot], ACT[rows, :], TT)

            def tile(j):
                slot = j % 2
                some = pl.ds(pl.multiple_of(j * LANES, LANES), LANES)
                wait(weights(0, j, j))

                @pl.when(j < NT_ - 1)
                def _():
                    start(weights(0, j + 1, j + 1))

                @pl.when(j == NT_ - 1)
                def _():
                    start(weights(1, 0, NT_))

                @pl.when(j > 0)
                def _():
                    wait(stores(j - 1, 0) + stores(j - 1, 1))

                @pl.when(j > 1)
                def _():
                    save(j - 2).wait()

                projections(0, slot)
                for c in range(0, T, 2 * LANES):
                    TB[slot, :, c : c + 2 * LANES] = A[c : c + 2 * LANES, some].T
                start(stores(j, 0))
                save(j).start()
                projections(1, slot)
                product(0)
                start(stores(j, 1))

                @pl.when(j == 0)
                def _():
                    load_dy.wait()

                down(lo, slot)
                product(1)
                turn(DD, some, DT)
                down(hi, slot)

            loop(NT_, tile)
            wait(stores(NT_ - 1, 0) + stores(NT_ - 1, 1))
            save(NT_ - 2).wait()
            save(NT_ - 1).wait()

        pl.run_scoped(forward, pltpu.VMEM((2, LANES, T), BF16))

        def norm_h(HB):
            n = T // CHUNK

            def save(i):
                return pltpu.make_async_copy(HB.at[i % 2], ht_s.at[i], iosem.at[i % 2])

            def part(i):
                r = columns_of(i)
                slot = i % 2

                @pl.when(i > 1)
                def _():
                    save(i - 2).wait()

                squares = []

                def add(rows):
                    h = (AT[rows, r].astype(F32) + ACC[rows, r].astype(BF16).astype(F32)).astype(BF16)
                    HB[slot, rows, :] = h
                    ACC[rows, r] = jnp.zeros((h.shape[0], CHUNK), F32)
                    wide = h.astype(F32)
                    squares.append(folded(wide * wide))

                down_rows(64, add)
                save(i).start()
                scale = lax.rsqrt(jnp.sum(sum(squares), axis=0, keepdims=True) / D + 1e-6)

                def norm(rows):
                    a = (HB[slot, rows, :].astype(F32) * scale).astype(BF16)
                    AT[rows, r] = a
                    A[r, rows] = a.T

                down_rows(LANES, norm)

            loop(n, part)
            save(n - 2).wait()
            save(n - 1).wait()

        pl.run_scoped(norm_h, pltpu.VMEM((2, D, CHUNK), BF16))
        pl.semaphore_wait(barrier, DEVICES - 1)

        def layer1(HB):
            def projections(half, slot):
                rows = lo if half == 0 else hi
                S[half][0][...] = dot(A[rows, :], WG[slot], NN)
                S[half][1][...] = dot(A[rows, :], WU[slot], NN)
                S[half][2][...] = dot(DD[rows, :], WD[slot], NT).astype(BF16)

            def back(half):
                g_ref, u_ref, d_ref = S[half]
                product_back(lambda r, n: g_ref[r : r + n, :], lambda r, n: u_ref[r : r + n, :], d_ref, half * H)

            def da(rows, slot):
                ACC[:, rows] += dot(WG[slot], DG[rows, :], NT)
                ACC[:, rows] += dot(WU[slot], DU[rows, :], NT)

            def tile(j):
                slot = (NT_ + j) % 2
                wait(weights(1, j, NT_ + j))

                @pl.when(j < NT_ - 1)
                def _():
                    start(weights(1, j + 1, NT_ + j + 1))

                @pl.when(j == NT_ - 1)
                def _():
                    start(weights(0, 0, 2 * NT_, True))

                projections(0, slot)
                projections(1, slot)
                back(0)
                apart(j > 0, lambda: sent(j - 1))
                da(lo, slot)
                back(1)
                da(hi, slot)
                apart(j == NT_ - 1, lambda: start([load_h(HB, 0), load_h(HB, 1), *loads(0)]))

                def gradients(i):
                    h = side_of(i)
                    for q in (0, 2):
                        put(2, h, dot(DT[q * R : (q + 2) * R, :], ACT[:, hidden_of(h)], NN), q)
                    for k, rhs in ((0, DG), (1, DU)):
                        put(k, h, dot(AT[half_of(h), :], rhs[...], NN))
                    apart(i == 0, lambda: send_far(j))

                loop(2, gradients)
                d2d(j, NEAR).start()
                keep(j).start()
                apart(j > 1, lambda: across(j - 2, True).wait_send())
                far_sum(j)
                across(j, True).start()

            loop(NT_, tile)
            norm_back(HB)

        pl.run_scoped(layer1, pltpu.VMEM((2, D, CHUNK), BF16))

    first_half()

    def layer0():
        S = ((G0, U0, D0), (G1, U1, D1))

        def tile(j):
            t = NT_ + j
            slot = j % 2
            half_sum = pl.ds(0, W)

            def back(half):
                g_ref, u_ref, d_ref = S[half]
                product_back(lambda r, n: g_ref[r : r + n, :], lambda r, n: u_ref[r : r + n, :], d_ref, half * H)

            wait(weights(0, j, 2 * NT_ + j, True))

            @pl.when(j < NT_ - 1)
            def _():
                start(weights(0, j + 1, 2 * NT_ + j + 1, True))

            wait(loads(j))
            D0[...] = dot(DD[lo, :], WD[slot], NT).astype(BF16)
            D1[...] = dot(DD[hi, :], WD[slot], NT).astype(BF16)
            back(0)
            ACC[:, half_sum] = dot(DT[:, lo], ACT[lo, :], NN)
            back(1)
            apart(j < NT_ - 1, lambda: start(loads(j + 1)))
            apart(j == 0, lambda: load_a0t.wait())
            apart(j > 0, lambda: sent(t - 1))

            def gradients(i):
                h = side_of(i)
                for q in (0, 2):
                    rows = slice(q * R, (q + 2) * R)
                    put(2, h, ACC[rows, hidden_of(h)] + dot(DT[rows, hi], ACT[hi, hidden_of(h)], NN), q)
                for k, rhs in ((0, DG), (1, DU)):
                    put(k, h, dot(AT[half_of(h), :], rhs[...], NN))
                apart((j > 1) & (i == 0), lambda: (far_store(t - 1).wait(), across(t - 1, False).start()))
                apart(i == 0, lambda: send_far(t))

            loop(2, gradients)
            d2d(t, NEAR).start()
            keep(t).start()
            apart(j < 3, lambda: across(t - 2, True).wait_send())
            far_sum(t)
            apart(j == 0, lambda: across(t, True).start())
            apart(j > 0, lambda: far_store(t).start())

        loop(NT_, tile)

    layer0()

    last = 2 * NT_ - 1
    far_store(last).wait()
    across(last, False).start()
    sent(last)
    pl.semaphore_wait(free, 1)

    def finish(DN):
        GN, UN, CB = GR.at[0, 1, 0], GR.at[0, 1, 1], GR.at[:, 0, 0]
        SQ[...] = jnp.zeros_like(SQ)

        def outs(t):
            l, j = 1 - t // NT_, t % NT_
            copies = []
            for p in range(DEVICES):
                copies.append(pltpu.make_async_copy(GN.at[:, pl.ds(p * LANES, LANES)], gg.at[l, :, columns(p, j)], fsem.at[3 + p]))
                copies.append(pltpu.make_async_copy(UN.at[:, pl.ds(p * LANES, LANES)], gu.at[l, :, columns(p, j)], fsem.at[7 + p]))
            rows = pl.ds(pl.multiple_of(j * LANES, LANES), LANES)
            copies.append(pltpu.make_async_copy(DN, gd.at[l, rows, :], fsem.at[11]))
            return copies

        def one(t):
            ins = [
                pltpu.make_async_copy(own.at[t], FB.at[0], fsem.at[0]),
                pltpu.make_async_copy(mate.at[t], FB.at[1], fsem.at[1]),
                pltpu.make_async_copy(cross.at[t], CB, fsem.at[2]),
            ]
            d2d(t, NEAR).wait_recv()
            start(ins[:2])
            across(t, False).wait_recv()
            ins[2].start()
            apart(t > NT_, lambda: across(t, False).wait_send())

            @pl.when(t > 0)
            def _():
                wait(outs(t - 1))

            wait(ins)
            for k in range(3):
                total = FB[0, k].astype(F32) + FB[1, k].astype(F32) + CB[k].astype(F32)
                g = total.astype(BF16)
                wide = g.astype(F32)
                SQ[...] += jnp.sum((wide * wide).reshape(R // 8, 8, W), axis=0)
                if k == 0:
                    GN[...] = g
                elif k == 1:
                    UN[...] = g
                else:
                    tall = jnp.concatenate([g[:, q * LANES : (q + 1) * LANES] for q in range(DEVICES)], axis=0)
                    DN[...] = tall.T
            start(outs(t))

        loop(2 * NT_, one)

        mine = jnp.sum(SQ[...], keepdims=True)
        SQS[DEVICES] = jnp.broadcast_to(mine, (8, LANES))
        copies = [
            pltpu.make_async_remote_copy(
                src_ref=SQS.at[DEVICES], dst_ref=SQS.at[me], send_sem=sq_send.at[k - 1], recv_sem=sq_recv.at[k - 1],
                device_id={"dp": (me + k) % DEVICES}, device_id_type=pl.DeviceIdType.MESH)
            for k in range(1, DEVICES)
        ]
        start(copies)
        SQS[me] = jnp.broadcast_to(mine, (8, LANES))
        wait(outs(last))
        for k in range(1, DEVICES):
            came = SQS.at[(me + DEVICES - k) % DEVICES]
            pltpu.make_async_copy(came, came, sq_recv.at[k - 1]).wait()
            copies[k - 1].wait_send()

    pl.run_scoped(finish, pltpu.VMEM((LANES, D), BF16))

    total = (SQS[0] + SQS[1]) + (SQS[2] + SQS[3])
    count = 2.0 * 3.0 * D * F
    factor[...] = jnp.minimum(1.0, 0.5 * lax.rsqrt(total / count + 1e-30))


def gradients(x, dy, wg, wu, wd):
    T, D = x.shape
    F = wg.shape[2]
    W = DEVICES * LANES
    n, R = F // W, D // DEVICES
    tiles = 2 * n
    hbm = lambda *s, d=BF16: jax.ShapeDtypeStruct(s, d)
    outs = [
        hbm(2, R, F), hbm(2, R, F), hbm(2, F // DEVICES, D), hbm(8, LANES, d=F32),
        hbm(n, T, W, d=F32), hbm(n, T, W, d=F32), hbm(D, T), hbm(T // CHUNK, D, CHUNK),
        hbm(tiles, 3, R, W), hbm(tiles, 3, R, W), hbm(tiles, 3, R, W), hbm(tiles, 3, R, W),
    ]
    sem = pltpu.SemaphoreType.DMA
    return pl.pallas_call(
        grads_kernel,
        out_shape=outs,
        in_specs=[ANY] * 5,
        out_specs=[ANY] * 3 + [pl.BlockSpec(memory_space=pltpu.VMEM)] + [ANY] * 8,
        scratch_shapes=[
            pltpu.VMEM((T, D), BF16), pltpu.VMEM((D, T), BF16), pltpu.VMEM((T, D), BF16), pltpu.VMEM((D, T), BF16),
            pltpu.VMEM((D, T), F32), pltpu.VMEM((3, 2, 2, R, W), BF16), *[pltpu.VMEM((T, W), BF16)] * 3,
            pltpu.VMEM((2, D, W), BF16), pltpu.VMEM((2, D, W), BF16), pltpu.VMEM((2, W, D), BF16),
            *[pltpu.VMEM((T // 2, W), F32), pltpu.VMEM((T // 2, W), F32), pltpu.VMEM((T // 2, W), BF16)] * 2,
            pltpu.VMEM((3, R, W), BF16), pltpu.VMEM((2, 3, R, W), BF16),
            pltpu.VMEM((8, W), F32), pltpu.VMEM((DEVICES + 1, 8, LANES), F32),
            sem((2, 3, DEVICES)), sem((7,)), sem((2,)), sem(()), sem((tiles,)), pltpu.SemaphoreType.REGULAR, sem(()), sem(()),
            sem((tiles,)), sem((tiles,)), sem((12,)), sem((DEVICES - 1,)), sem((DEVICES - 1,)),
        ],
        compiler_params=pltpu.CompilerParams(collective_id=0, has_side_effects=True, vmem_limit_bytes=VMEM_BYTES),
        name="gradients",
    )(x, dy, wg, wu, wd)[:4]


def adamw_kernel(me, factor, g, w, m, v, *refs):
    out, send, new_m, new_v, turn = refs[-5:]
    turn[0] = me[0]
    some = 32

    def part(i):
        r = pl.ds(pl.multiple_of(i * some, some), some)
        grad = g[r, :].astype(F32) * factor[0:1, 0:1]
        one = 0.9 * m[r, :] + 0.1 * grad
        two = 0.95 * v[r, :] + 0.05 * grad * grad
        wide = w[r, :].astype(F32)
        new_w = (wide - 0.02 * (one * lax.rsqrt(two + 1e-8) + 0.1 * wide)).astype(BF16)
        out[r, :] = new_w
        send[r, :] = new_w
        new_m[r, :] = one
        new_v[r, :] = two

    loop(m.shape[0] // some, part)


def adamw(me, factor, g, w, m, v, so_far, layer, first, steps, by_columns):
    rows = m.shape[1] if by_columns else LANES
    cols = DEVICES * LANES if by_columns else m.shape[2]
    tile = (None, rows, cols)
    if by_columns:
        block = pl.BlockSpec(tile, lambda i, me: (layer, 0, first + i))
        whole = pl.BlockSpec(tile, lambda i, me: (layer, me[0], first + i))
        alone, send = (rows, steps * cols), pl.BlockSpec((rows, cols), lambda i, me: (0, i))
    else:
        n = m.shape[1] // LANES
        block = pl.BlockSpec(tile, lambda i, me: (layer, first + i, 0))
        whole = pl.BlockSpec(tile, lambda i, me: (layer, me[0] * n + first + i, 0))
        alone, send = (steps * rows, cols), pl.BlockSpec((rows, cols), lambda i, me: (i, 0))
    begun = so_far is not None
    shape = lambda a: jax.ShapeDtypeStruct(a.shape, a.dtype)
    out, sent, new_m, new_v, turn = pl.pallas_call(
        adamw_kernel,
        grid_spec=pltpu.PrefetchScalarGridSpec(
            num_scalar_prefetch=1,
            grid=(steps,),
            in_specs=[pl.BlockSpec((8, LANES), lambda i, me: (0, 0)), block, whole, block, block] + [ANY] * (3 * begun),
            out_specs=[whole, send, block, block, pl.BlockSpec(memory_space=pltpu.SMEM)],
        ),
        out_shape=[shape(w), jax.ShapeDtypeStruct(alone, BF16), shape(m), shape(v), shape(me)],
        input_output_aliases={6: 0, 7: 2, 8: 3} if begun else {},
        compiler_params=pltpu.CompilerParams(vmem_limit_bytes=VMEM_BYTES),
        cost_estimate=pl.CostEstimate(flops=20 * steps * rows * cols, bytes_accessed=28 * steps * rows * cols, transcendentals=0),
        name="adamw",
    )(me, factor, g, w, m, v, *(so_far or ()))
    return (out, new_m, new_v), sent, turn


def place_kernel(n, at, me_ref, _, *refs):
    pieces, out, turn, bufs, sems = refs[:n], refs[n], refs[n + 1], refs[n + 2 : 2 * n + 2], refs[2 * n + 2]
    turn[0] = me_ref[0]
    loads = [pltpu.make_async_copy(p, b, sems.at[0, k]) for k, (p, b) in enumerate(zip(pieces, bufs))]
    for c in loads:
        c.start()
    stores = []
    for k in range(n):
        loads[k].wait()
        stores.append(pltpu.make_async_copy(bufs[k], out.at[at(k, me_ref[0])], sems.at[1, k]))
        stores[k].start()
    for c in stores:
        c.wait()


def place(out, me, pieces, owners, layer, first, by_columns):
    rows, cols = pieces[0].shape

    def at(k, me):
        owner = me ^ owners[k]
        if by_columns:
            return layer, pl.ds(pl.multiple_of(owner * rows, 8), rows), pl.ds(first * DEVICES * LANES, cols)
        return layer, pl.ds(pl.multiple_of(owner * (out.shape[1] // DEVICES) + first * LANES, LANES), rows), slice(None)

    n = len(pieces)
    return pl.pallas_call(
        functools.partial(place_kernel, n, at),
        in_specs=[pl.BlockSpec(memory_space=pltpu.SMEM)] + [ANY] * (n + 1),
        out_specs=[ANY, pl.BlockSpec(memory_space=pltpu.SMEM)],
        out_shape=[jax.ShapeDtypeStruct(out.shape, out.dtype), jax.ShapeDtypeStruct(me.shape, me.dtype)],
        scratch_shapes=[pltpu.VMEM((rows, cols), BF16)] * n + [pltpu.SemaphoreType.DMA((2, n))],
        input_output_aliases={1: 0},
        compiler_params=pltpu.CompilerParams(vmem_limit_bytes=VMEM_BYTES),
        cost_estimate=pl.CostEstimate(flops=4 * n * rows * cols, bytes_accessed=4 * n * rows * cols, transcendentals=0),
        name="place",
    )(me, out, *pieces)


def other_chip(a):
    return lax.ppermute(a, "dp", [(i, i ^ 2) for i in range(4)])


def other_core(a):
    return lax.ppermute(a, "dp", [(i, i ^ 1) for i in range(4)])


CHUNKS = (
    (0, 0, 0, 1), (0, 0, 1, 3), (0, 0, 4, 5), (0, 1, 0, 9), (1, 0, 0, 9), (1, 1, 0, 9), (2, 0, 0, 9), (2, 1, 0, 5), (2, 1, 5, 3), (2, 1, 8, 1),
)


def solution(mesh):
    def step(x, dy, *arrays):
        weights, m, v = (arrays[i : i + 3] for i in (0, 3, 6))
        me = lax.axis_index("dp").astype(jnp.int32).reshape(1)
        *g, factor = gradients(x[0], dy[0], *weights)
        new = [None] * 3
        gathered = []
        for k, layer, first, steps in CHUNKS:
            new[k], sent, me = adamw(me, factor, g[k], weights[k], m[k], v[k], new[k], layer, first, steps, k < 2)
            far = other_chip(sent)
            own = other_core(sent)
            gathered.append((far, own, other_core(far)))
        whole = [n[0] for n in new]
        for (k, layer, first, steps), pieces in zip(CHUNKS, gathered):
            whole[k], me = place(whole[k], me, pieces, (2, 1, 3), layer, first, k < 2)
        return (*whole, *(n[1] for n in new), *(n[2] for n in new))

    rows = P(None, "dp", None)
    return jax.shard_map(
        step,
        mesh=mesh,
        in_specs=(P(("rep", "dp")), P(("rep", "dp")), *(P(),) * 3, *(rows,) * 6),
        out_specs=(*(P("rep"),) * 3, *(P("rep", "dp"),) * 6),
        check_vma=False,
    )
```

```python
import functools

import jax
import jax.numpy as jnp
from jax import lax
from jax.experimental import pallas as pl
from jax.experimental.pallas import tpu as pltpu
from jax.sharding import PartitionSpec as P


F32, BF16 = jnp.float32, jnp.bfloat16
DEVICES = 4
LANES = 128
CHUNK = 256
EARLY = 3
ANY = pl.BlockSpec(memory_space=pl.ANY)
VMEM_BYTES = 67_043_328


def dot(a, b, dims):
    return lax.dot_general(a, b, (dims, ((), ())), preferred_element_type=F32)


NN, NT, TT = ((1,), (0,)), ((1,), (1,)), ((0,), (1,))


def sigmoid(x):
    return 1.0 / (1.0 + jnp.exp(-x))


def loop(n, body):
    lax.fori_loop(0, n, lambda i, c: (body(i), c)[1], 0)


def apart(cond, body):
    lax.fori_loop(0, jnp.where(cond, 1, 0), lambda i, c: (body(), c)[1], 0)


def grads_kernel(
    x, dy, wg, wu, wd, md, vd,
    gg, gu, gd, factor, mo, vo, go, ge, gate_s, up_s, a0t_s, ht_s, mate, own, far, cross,
    DN, A, AT, DD, DT, ACC, GR, ACT, DG, DU, WG, WU, WD, G0, U0, D0, G1, U1, D1, MATEB, FB, SQ, SQS,
    wsem, iosem, d2d_send, d2d_recv, near_recv, free, own_sem, far_sem, x_send, x_recv, fsem, sq_send, sq_recv, e_sem, e_send, e_recv,
):
    T, D = x.shape
    F = wg.shape[2]
    W = DEVICES * LANES
    NT_ = F // W
    FAR, NEAR = 0, 1
    H = T // 2
    R = D // DEVICES
    me = lax.axis_index("dp")
    chip, core = me // 2, me % 2
    mate_id, cross_id = {"dp": chip * 2 + 1 - core}, {"dp": (1 - chip) * 2 + core}
    lo, hi = pl.ds(0, H), pl.ds(H, H)

    barrier = pltpu.get_barrier_semaphore()
    for k in range(1, DEVICES):
        pl.semaphore_signal(barrier, inc=1, device_id={"dp": (me + k) % DEVICES}, device_id_type=pl.DeviceIdType.MESH)

    def columns(p, j):
        return pl.ds(pl.multiple_of(p * (F // DEVICES) + j * LANES, LANES), LANES)

    def weights(l, j, q, down_only=False):
        slot = q % 2
        copies = []
        for p in range(DEVICES):
            piece = pl.ds(p * LANES, LANES)
            if not down_only:
                copies.append(pltpu.make_async_copy(wg.at[l, :, columns(p, j)], WG.at[slot, :, piece], wsem.at[slot, 0, p]))
                copies.append(pltpu.make_async_copy(wu.at[l, :, columns(p, j)], WU.at[slot, :, piece], wsem.at[slot, 1, p]))
            copies.append(pltpu.make_async_copy(wd.at[l, columns(p, j), :], WD.at[slot, piece, :], wsem.at[slot, 2, p]))
        return copies

    def start(copies):
        for c in copies:
            c.start()

    def wait(copies):
        for c in copies:
            c.wait()

    def owner_chip(side):
        return 1 - chip if side == FAR else chip

    def d2d(t, side):
        return pltpu.make_async_remote_copy(
            src_ref=GR.at[:, owner_chip(side), 1 - core], dst_ref=MATEB if side == FAR else mate.at[t],
            send_sem=d2d_send.at[side], recv_sem=d2d_recv if side == FAR else near_recv.at[t],
            device_id=mate_id, device_id_type=pl.DeviceIdType.MESH)

    def keep(t):
        return pltpu.make_async_copy(GR.at[:, chip, core], own.at[t], own_sem)

    def across(t, direct):
        return pltpu.make_async_remote_copy(
            src_ref=FB.at[t % 2] if direct else far.at[t], dst_ref=cross.at[t], send_sem=x_send.at[t], recv_sem=x_recv.at[t],
            device_id=cross_id, device_id_type=pl.DeviceIdType.MESH)

    def moments():
        rows = pl.ds(0, EARLY * LANES)
        return [
            pltpu.make_async_remote_copy(
                src_ref=src.at[1, rows], dst_ref=dst, send_sem=e_send.at[n], recv_sem=e_recv.at[n],
                device_id=cross_id, device_id_type=pl.DeviceIdType.MESH)
            for n, (src, dst) in enumerate(((md, mo), (vd, vo)))
        ]

    def early_rows(t):
        return pl.ds(pl.multiple_of(t * LANES, LANES), LANES)

    def early_send(t):
        return pltpu.make_async_remote_copy(
            src_ref=ge.at[early_rows(t)], dst_ref=go.at[early_rows(t)], send_sem=e_send.at[2 + t], recv_sem=e_recv.at[2 + t],
            device_id=cross_id, device_id_type=pl.DeviceIdType.MESH)

    def early_store(t):
        return pltpu.make_async_copy(DN, ge.at[early_rows(t)], e_sem.at[3])

    def early_loads(t):
        return [
            pltpu.make_async_copy(src.at[t, 2], D0.at[pl.ds(n * R, R)], e_sem.at[n]) for n, src in enumerate((own, mate, cross))
        ]

    def early_begin(t):
        across(t, True).wait_recv()
        d2d(t, NEAR).wait_recv()
        start(early_loads(t))

    def early_sum(t):
        wait(early_loads(t))
        g = (D0[0:R, :].astype(F32) + D0[R : 2 * R, :].astype(F32) + D0[2 * R : 3 * R, :].astype(F32)).astype(BF16)
        DN[...] = tall(g).T
        early_store(t).start()

    def tall(g):
        return jnp.concatenate([g[:, q * LANES : (q + 1) * LANES] for q in range(DEVICES)], axis=0)

    def far_store(t):
        return pltpu.make_async_copy(FB.at[t % 2], far.at[t], far_sem)

    def send_far(t):
        pl.when(t > 0)(lambda: pl.semaphore_wait(free, 1))
        d2d(t, FAR).start()

    def far_sum(t):
        d2d(t, FAR).wait_recv()

        def some(i):
            rows = pl.ds(pl.multiple_of(i * 96, 96), 96)
            for k in range(3):
                FB[t % 2, k, rows, :] = (GR[k, 1 - chip, core, rows, :].astype(F32) + MATEB[k, rows, :].astype(F32)).astype(BF16)

        loop(R // 96, some)
        pl.semaphore_signal(free, inc=1, device_id=mate_id, device_id_type=pl.DeviceIdType.MESH)

    def sent(t):
        d2d(t, FAR).wait_send()
        d2d(t, NEAR).wait_send()
        keep(t).wait()

    def put(k, h, value, first=0):
        value = value.astype(BF16)
        for o in range(2):
            if k < 2:
                GR[k, h, o] = value[o * R : (o + 1) * R]
            else:
                for q in range(value.shape[0] // R):
                    lanes = slice((first + q) * LANES, (first + q + 1) * LANES)
                    GR[k, h, o, :, lanes] = value[q * R : (q + 1) * R, o * LANES : (o + 1) * LANES]

    def side_of(i):
        return jnp.where(i == 0, 1 - chip, chip)

    def hidden_of(h):
        return pl.ds(pl.multiple_of(h * (W // 2), W // 2), W // 2)

    def half_of(i):
        return pl.ds(pl.multiple_of(i * (D // 2), D // 2), D // 2)

    def product_back(g_ref, u_ref, d_ref, r0):
        step = 16
        for r in range(0, H, step):
            g, u = g_ref(r, step), u_ref(r, step)
            d = d_ref[r : r + step, :].astype(F32)
            s = sigmoid(g)
            si = g * s
            ACT[r0 + r : r0 + r + step, :] = (si * u).astype(BF16)
            DU[r0 + r : r0 + r + step, :] = (d * si).astype(BF16)
            DG[r0 + r : r0 + r + step, :] = (d * u * (s + si * (1.0 - s))).astype(BF16)

    def columns_of(i):
        return pl.ds(pl.multiple_of(i * CHUNK, CHUNK), CHUNK)

    def down_rows(step, body):
        for r in range(0, D, step):
            body(slice(r, r + step))

    def folded(t):
        return jnp.sum(t.reshape(t.shape[0] // 8, 8, t.shape[1]), axis=0)

    def turn(src, rows, dst):
        for c in range(0, T, 2 * LANES):
            dst[rows, c : c + 2 * LANES] = src[c : c + 2 * LANES, rows].T

    def loads(j):
        return [
            pltpu.make_async_copy(to.at[j, pl.ds(half * H, H), :], ref, iosem.at[3 + 2 * half + n])
            for half, refs in enumerate(((G0, U0), (G1, U1)))
            for n, (ref, to) in enumerate(zip(refs, (gate_s, up_s)))
        ]

    def load_h(HB, i):
        return pltpu.make_async_copy(ht_s.at[i], HB.at[i % 2], iosem.at[1 + i % 2])

    load_a0t = pltpu.make_async_copy(a0t_s, AT, iosem.at[0])

    def norm_back(HB):
        n = T // CHUNK

        def part(i):
            r = columns_of(i)
            slot = i % 2
            load_h(HB, i).wait()

            squares, along = [], []

            def add(rows):
                wide = HB[slot, rows, :].astype(F32)
                squares.append(folded(wide * wide))
                along.append(folded(ACC[rows, r].astype(BF16).astype(F32) * wide))

            down_rows(64, add)
            scale = lax.rsqrt(jnp.sum(sum(squares), axis=0, keepdims=True) / D + 1e-6)
            shrink = jnp.sum(sum(along), axis=0, keepdims=True) / D * (scale * scale * scale)

            def back(rows):
                wide = HB[slot, rows, :].astype(F32)
                dwide = ACC[rows, r].astype(BF16).astype(F32) * scale - wide * shrink
                dh = (DT[rows, r].astype(F32) + dwide.astype(BF16).astype(F32)).astype(BF16)
                DT[rows, r] = dh
                DD[r, rows] = dh.T

            down_rows(LANES, back)
            apart(i < n - 2, lambda: load_h(HB, i + 2).start())

        loop(n, part)
        sent(NT_ - 1)
        load_a0t.start()

    def first_half():
        S = ((G0, U0, D0), (G1, U1, D1))

        def forward(TB):
            load_x = [pltpu.make_async_copy(x.at[pl.ds(c * (T // 4), T // 4)], DD.at[pl.ds(c * (T // 4), T // 4)], iosem.at[c]) for c in range(4)]
            start(load_x)
            start(weights(0, 0, 0))

            def zero(i):
                ACC[pl.ds(pl.multiple_of(i * LANES, LANES), LANES), :] = jnp.zeros((LANES, T), F32)

            loop(D // LANES, zero)

            def norm_x(i):
                r = pl.ds(pl.multiple_of(i * LANES, LANES), LANES)
                wide = DD[r, :].astype(F32)
                A[r, :] = (wide * lax.rsqrt(jnp.mean(wide * wide, axis=1, keepdims=True) + 1e-6)).astype(BF16)
                AT[:, r] = DD[r, :].T

            for c in range(4):
                load_x[c].wait()
                loop(T // 4 // LANES, lambda i, c=c: norm_x(c * (T // 4 // LANES) + i))
            load_dy = pltpu.make_async_copy(dy, DD, iosem.at[6])
            load_dy.start()
            pl.semaphore_wait(barrier, DEVICES - 1)
            start(moments())

            def stores(j, half):
                return [
                    pltpu.make_async_copy(ref, to.at[j, pl.ds(half * H, H), :], iosem.at[2 * half + n])
                    for n, (ref, to) in enumerate(zip(S[half][:2], (gate_s, up_s)))
                ]

            def save(j):
                return pltpu.make_async_copy(TB.at[j % 2], a0t_s.at[pl.ds(pl.multiple_of(j * LANES, LANES), LANES), :], iosem.at[4 + j % 2])

            def projections(half, slot):
                rows = lo if half == 0 else hi
                S[half][0][...] = dot(A[rows, :], WG[slot], NN)
                S[half][1][...] = dot(A[rows, :], WU[slot], NN)

            def product(half):
                g_ref, u_ref, _ = S[half]
                for r in range(0, H, 16):
                    g = g_ref[r : r + 16, :]
                    ACT[half * H + r : half * H + r + 16, :] = (g * sigmoid(g) * u_ref[r : r + 16, :]).astype(BF16)

            def down(rows, slot):
                ACC[:, rows] += dot(WD[slot], ACT[rows, :], TT)

            def tile(j):
                slot = j % 2
                some = pl.ds(pl.multiple_of(j * LANES, LANES), LANES)
                wait(weights(0, j, j))

                @pl.when(j < NT_ - 1)
                def _():
                    start(weights(0, j + 1, j + 1))

                @pl.when(j == NT_ - 1)
                def _():
                    start(weights(1, 0, NT_))

                @pl.when(j > 0)
                def _():
                    wait(stores(j - 1, 0) + stores(j - 1, 1))

                @pl.when(j > 1)
                def _():
                    save(j - 2).wait()

                projections(0, slot)
                for c in range(0, T, 2 * LANES):
                    TB[slot, :, c : c + 2 * LANES] = A[c : c + 2 * LANES, some].T
                start(stores(j, 0))
                save(j).start()
                projections(1, slot)
                product(0)
                start(stores(j, 1))

                @pl.when(j == 0)
                def _():
                    load_dy.wait()

                down(lo, slot)
                product(1)
                turn(DD, some, DT)
                down(hi, slot)

            loop(NT_, tile)
            wait(stores(NT_ - 1, 0) + stores(NT_ - 1, 1))
            save(NT_ - 2).wait()
            save(NT_ - 1).wait()

        pl.run_scoped(forward, pltpu.VMEM((2, LANES, T), BF16))

        def norm_h(HB):
            n = T // CHUNK

            def save(i):
                return pltpu.make_async_copy(HB.at[i % 2], ht_s.at[i], iosem.at[i % 2])

            def part(i):
                r = columns_of(i)
                slot = i % 2

                @pl.when(i > 1)
                def _():
                    save(i - 2).wait()

                squares = []

                def add(rows):
                    h = (AT[rows, r].astype(F32) + ACC[rows, r].astype(BF16).astype(F32)).astype(BF16)
                    HB[slot, rows, :] = h
                    ACC[rows, r] = jnp.zeros((h.shape[0], CHUNK), F32)
                    wide = h.astype(F32)
                    squares.append(folded(wide * wide))

                down_rows(64, add)
                save(i).start()
                scale = lax.rsqrt(jnp.sum(sum(squares), axis=0, keepdims=True) / D + 1e-6)

                def norm(rows):
                    a = (HB[slot, rows, :].astype(F32) * scale).astype(BF16)
                    AT[rows, r] = a
                    A[r, rows] = a.T

                down_rows(LANES, norm)

            loop(n, part)
            save(n - 2).wait()
            save(n - 1).wait()

        pl.run_scoped(norm_h, pltpu.VMEM((2, D, CHUNK), BF16))

        def layer1(HB):
            def projections(half, slot):
                rows = lo if half == 0 else hi
                S[half][0][...] = dot(A[rows, :], WG[slot], NN)
                S[half][1][...] = dot(A[rows, :], WU[slot], NN)
                S[half][2][...] = dot(DD[rows, :], WD[slot], NT).astype(BF16)

            def back(half):
                g_ref, u_ref, d_ref = S[half]
                product_back(lambda r, n: g_ref[r : r + n, :], lambda r, n: u_ref[r : r + n, :], d_ref, half * H)

            def da(rows, slot):
                ACC[:, rows] += dot(WG[slot], DG[rows, :], NT)
                ACC[:, rows] += dot(WU[slot], DU[rows, :], NT)

            def tile(j):
                slot = (NT_ + j) % 2
                wait(weights(1, j, NT_ + j))

                @pl.when(j < NT_ - 1)
                def _():
                    start(weights(1, j + 1, NT_ + j + 1))

                @pl.when(j == NT_ - 1)
                def _():
                    start(weights(0, 0, 2 * NT_, True))

                projections(0, slot)
                projections(1, slot)
                back(0)
                apart(j > 0, lambda: sent(j - 1))
                apart((j > 2) & (j < 3 + EARLY), lambda: (early_store(j - 3).wait(), early_send(j - 3).start()))
                apart((j > 1) & (j < 2 + EARLY), lambda: early_begin(j - 2))
                da(lo, slot)
                back(1)
                da(hi, slot)
                apart(j == NT_ - 1, lambda: start([load_h(HB, 0), load_h(HB, 1), *loads(0)]))

                def gradients(i):
                    h = side_of(i)
                    for q in (0, 2):
                        put(2, h, dot(DT[q * R : (q + 2) * R, :], ACT[:, hidden_of(h)], NN), q)
                    for k, rhs in ((0, DG), (1, DU)):
                        put(k, h, dot(AT[half_of(h), :], rhs[...], NN))
                    apart(i == 0, lambda: send_far(j))

                loop(2, gradients)
                d2d(j, NEAR).start()
                keep(j).start()
                apart(j > 1, lambda: across(j - 2, True).wait_send())
                far_sum(j)
                across(j, True).start()
                apart((j > 1) & (j < 2 + EARLY), lambda: early_sum(j - 2))

            loop(NT_, tile)
            norm_back(HB)

        pl.run_scoped(layer1, pltpu.VMEM((2, D, CHUNK), BF16))

    first_half()

    def layer0():
        S = ((G0, U0, D0), (G1, U1, D1))

        def tile(j):
            t = NT_ + j
            slot = j % 2
            half_sum = pl.ds(0, W)

            def back(half):
                g_ref, u_ref, d_ref = S[half]
                product_back(lambda r, n: g_ref[r : r + n, :], lambda r, n: u_ref[r : r + n, :], d_ref, half * H)

            wait(weights(0, j, 2 * NT_ + j, True))

            @pl.when(j < NT_ - 1)
            def _():
                start(weights(0, j + 1, 2 * NT_ + j + 1, True))

            wait(loads(j))
            D0[...] = dot(DD[lo, :], WD[slot], NT).astype(BF16)
            D1[...] = dot(DD[hi, :], WD[slot], NT).astype(BF16)
            back(0)
            ACC[:, half_sum] = dot(DT[:, lo], ACT[lo, :], NN)
            back(1)
            apart(j < NT_ - 1, lambda: start(loads(j + 1)))
            apart(j == 0, lambda: load_a0t.wait())
            apart(j > 0, lambda: sent(t - 1))

            def gradients(i):
                h = side_of(i)
                for q in (0, 2):
                    rows = slice(q * R, (q + 2) * R)
                    put(2, h, ACC[rows, hidden_of(h)] + dot(DT[rows, hi], ACT[hi, hidden_of(h)], NN), q)
                for k, rhs in ((0, DG), (1, DU)):
                    put(k, h, dot(AT[half_of(h), :], rhs[...], NN))
                apart((j > 1) & (i == 0), lambda: (far_store(t - 1).wait(), across(t - 1, False).start()))
                apart(i == 0, lambda: send_far(t))

            loop(2, gradients)
            d2d(t, NEAR).start()
            keep(t).start()
            apart(j < 3, lambda: across(t - 2, True).wait_send())
            far_sum(t)
            apart(j == 0, lambda: across(t, True).start())
            apart(j > 0, lambda: far_store(t).start())

        loop(NT_, tile)

    layer0()

    last = 2 * NT_ - 1
    far_store(last).wait()
    across(last, False).start()
    sent(last)
    pl.semaphore_wait(free, 1)

    def finish():
        GN, UN, CB = GR.at[0, 1, 0], GR.at[0, 1, 1], GR.at[:, 0, 0]
        SQ[...] = jnp.zeros_like(SQ)

        def outs(t):
            l, j = 1 - t // NT_, t % NT_
            copies = []
            for p in range(DEVICES):
                copies.append(pltpu.make_async_copy(GN.at[:, pl.ds(p * LANES, LANES)], gg.at[l, :, columns(p, j)], fsem.at[3 + p]))
                copies.append(pltpu.make_async_copy(UN.at[:, pl.ds(p * LANES, LANES)], gu.at[l, :, columns(p, j)], fsem.at[7 + p]))
            rows = pl.ds(pl.multiple_of(j * LANES, LANES), LANES)
            copies.append(pltpu.make_async_copy(DN, gd.at[l, rows, :], fsem.at[11]))
            return copies

        def one(t):
            ins = [
                pltpu.make_async_copy(own.at[t], FB.at[0], fsem.at[0]),
                pltpu.make_async_copy(mate.at[t], FB.at[1], fsem.at[1]),
                pltpu.make_async_copy(cross.at[t], CB, fsem.at[2]),
            ]
            apart(t >= EARLY, lambda: d2d(t, NEAR).wait_recv())
            start(ins[:2])
            apart(t >= EARLY, lambda: across(t, False).wait_recv())
            ins[2].start()
            apart(t > NT_, lambda: across(t, False).wait_send())

            @pl.when(t > 0)
            def _():
                wait(outs(t - 1))

            wait(ins)
            for k in range(3):
                total = FB[0, k].astype(F32) + FB[1, k].astype(F32) + CB[k].astype(F32)
                g = total.astype(BF16)
                wide = g.astype(F32)
                SQ[...] += jnp.sum((wide * wide).reshape(R // 8, 8, W), axis=0)
                if k == 0:
                    GN[...] = g
                elif k == 1:
                    UN[...] = g
                else:
                    DN[...] = tall(g).T
            start(outs(t))

        loop(2 * NT_, one)

        mine = jnp.sum(SQ[...], keepdims=True)
        SQS[DEVICES] = jnp.broadcast_to(mine, (8, LANES))
        copies = [
            pltpu.make_async_remote_copy(
                src_ref=SQS.at[DEVICES], dst_ref=SQS.at[me], send_sem=sq_send.at[k - 1], recv_sem=sq_recv.at[k - 1],
                device_id={"dp": (me + k) % DEVICES}, device_id_type=pl.DeviceIdType.MESH)
            for k in range(1, DEVICES)
        ]
        start(copies)
        SQS[me] = jnp.broadcast_to(mine, (8, LANES))
        wait(outs(last))
        for k in range(1, DEVICES):
            came = SQS.at[(me + DEVICES - k) % DEVICES]
            pltpu.make_async_copy(came, came, sq_recv.at[k - 1]).wait()
            copies[k - 1].wait_send()

    finish()
    for c in moments():
        c.wait()
    for t in range(EARLY):
        early_send(t).wait()

    total = (SQS[0] + SQS[1]) + (SQS[2] + SQS[3])
    count = 2.0 * 3.0 * D * F
    factor[...] = jnp.minimum(1.0, 0.5 * lax.rsqrt(total / count + 1e-30))


def gradients(x, dy, wg, wu, wd, md, vd):
    T, D = x.shape
    F = wg.shape[2]
    W = DEVICES * LANES
    n, R = F // W, D // DEVICES
    tiles = 2 * n
    hbm = lambda *s, d=BF16: jax.ShapeDtypeStruct(s, d)
    outs = [
        hbm(2, R, F), hbm(2, R, F), hbm(2, F // DEVICES, D), hbm(8, LANES, d=F32),
        hbm(EARLY * LANES, D, d=F32), hbm(EARLY * LANES, D, d=F32), hbm(EARLY * LANES, D), hbm(EARLY * LANES, D),
        hbm(n, T, W, d=F32), hbm(n, T, W, d=F32), hbm(D, T), hbm(T // CHUNK, D, CHUNK),
        hbm(tiles, 3, R, W), hbm(tiles, 3, R, W), hbm(tiles, 3, R, W), hbm(tiles, 3, R, W),
    ]
    sem = pltpu.SemaphoreType.DMA
    return pl.pallas_call(
        grads_kernel,
        out_shape=outs,
        in_specs=[ANY] * 7,
        out_specs=[ANY] * 3 + [pl.BlockSpec(memory_space=pltpu.VMEM)] + [ANY] * 12,
        scratch_shapes=[
            pltpu.VMEM((LANES, D), BF16),
            pltpu.VMEM((T, D), BF16), pltpu.VMEM((D, T), BF16), pltpu.VMEM((T, D), BF16), pltpu.VMEM((D, T), BF16),
            pltpu.VMEM((D, T), F32), pltpu.VMEM((3, 2, 2, R, W), BF16), *[pltpu.VMEM((T, W), BF16)] * 3,
            pltpu.VMEM((2, D, W), BF16), pltpu.VMEM((2, D, W), BF16), pltpu.VMEM((2, W, D), BF16),
            *[pltpu.VMEM((T // 2, W), F32), pltpu.VMEM((T // 2, W), F32), pltpu.VMEM((T // 2, W), BF16)] * 2,
            pltpu.VMEM((3, R, W), BF16), pltpu.VMEM((2, 3, R, W), BF16),
            pltpu.VMEM((8, W), F32), pltpu.VMEM((DEVICES + 1, 8, LANES), F32),
            sem((2, 3, DEVICES)), sem((7,)), sem((2,)), sem(()), sem((tiles,)), pltpu.SemaphoreType.REGULAR, sem(()), sem(()),
            sem((tiles,)), sem((tiles,)), sem((12,)), sem((DEVICES - 1,)), sem((DEVICES - 1,)),
            sem((4,)), sem((2 + EARLY,)), sem((2 + EARLY,)),
        ],
        compiler_params=pltpu.CompilerParams(collective_id=0, has_side_effects=True, vmem_limit_bytes=VMEM_BYTES),
        name="gradients",
    )(x, dy, wg, wu, wd, md, vd)[:7]


def adamw_kernel(me, factor, g, w, m, v, *refs):
    out, send, new_m, new_v, turn = refs[-5:]
    turn[0] = me[0]
    some = 32

    def part(i):
        r = pl.ds(pl.multiple_of(i * some, some), some)
        grad = g[r, :].astype(F32) * factor[0:1, 0:1]
        one = 0.9 * m[r, :] + 0.1 * grad
        two = 0.95 * v[r, :] + 0.05 * grad * grad
        wide = w[r, :].astype(F32)
        new_w = (wide - 0.02 * (one * lax.rsqrt(two + 1e-8) + 0.1 * wide)).astype(BF16)
        out[r, :] = new_w
        send[r, :] = new_w
        new_m[r, :] = one
        new_v[r, :] = two

    loop(m.shape[0] // some, part)


def adamw(me, factor, g, w, m, v, so_far, layer, first, steps, by_columns):
    rows = m.shape[1] if by_columns else LANES
    cols = DEVICES * LANES if by_columns else m.shape[2]
    tile = (None, rows, cols)
    if by_columns:
        block = pl.BlockSpec(tile, lambda i, me: (layer, 0, first + i))
        whole = pl.BlockSpec(tile, lambda i, me: (layer, me[0], first + i))
        alone, send = (rows, steps * cols), pl.BlockSpec((rows, cols), lambda i, me: (0, i))
    else:
        n = m.shape[1] // LANES
        block = pl.BlockSpec(tile, lambda i, me: (layer, first + i, 0))
        whole = pl.BlockSpec(tile, lambda i, me: (layer, me[0] * n + first + i, 0))
        alone, send = (steps * rows, cols), pl.BlockSpec((rows, cols), lambda i, me: (i, 0))
    begun = so_far is not None
    shape = lambda a: jax.ShapeDtypeStruct(a.shape, a.dtype)
    out, sent, new_m, new_v, turn = pl.pallas_call(
        adamw_kernel,
        grid_spec=pltpu.PrefetchScalarGridSpec(
            num_scalar_prefetch=1,
            grid=(steps,),
            in_specs=[pl.BlockSpec((8, LANES), lambda i, me: (0, 0)), block, whole, block, block] + [ANY] * (3 * begun),
            out_specs=[whole, send, block, block, pl.BlockSpec(memory_space=pltpu.SMEM)],
        ),
        out_shape=[shape(w), jax.ShapeDtypeStruct(alone, BF16), shape(m), shape(v), shape(me)],
        input_output_aliases={6: 0, 7: 2, 8: 3} if begun else {},
        compiler_params=pltpu.CompilerParams(vmem_limit_bytes=VMEM_BYTES),
        cost_estimate=pl.CostEstimate(flops=20 * steps * rows * cols, bytes_accessed=28 * steps * rows * cols, transcendentals=0),
        name="adamw",
    )(me, factor, g, w, m, v, *(so_far or ()))
    return (out, new_m, new_v), sent, turn


def other_kernel(me, factor, g, w, m, v, _, out, send, turn):
    turn[0] = me[0]
    grad = g[...].astype(F32) * factor[0:1, 0:1]
    one = 0.9 * m[...] + 0.1 * grad
    two = 0.95 * v[...] + 0.05 * grad * grad
    wide = w[...].astype(F32)
    new_w = (wide - 0.02 * (one * lax.rsqrt(two + 1e-8) + 0.1 * wide)).astype(BF16)
    out[...] = new_w
    send[...] = new_w


def adamw_of_other(me, factor, g, w, m, v, out, layer):
    D = m.shape[1]
    n = w.shape[1] // DEVICES // LANES
    block = pl.BlockSpec((LANES, D), lambda i, me: (i, 0))
    whole = pl.BlockSpec((None, LANES, D), lambda i, me: (layer, (me[0] ^ 2) * n + i, 0))
    return pl.pallas_call(
        other_kernel,
        grid_spec=pltpu.PrefetchScalarGridSpec(
            num_scalar_prefetch=1,
            grid=(EARLY,),
            in_specs=[pl.BlockSpec((8, LANES), lambda i, me: (0, 0)), block, whole, block, block, ANY],
            out_specs=[whole, block, pl.BlockSpec(memory_space=pltpu.SMEM)],
        ),
        out_shape=[jax.ShapeDtypeStruct(w.shape, BF16), jax.ShapeDtypeStruct(m.shape, BF16), jax.ShapeDtypeStruct(me.shape, me.dtype)],
        input_output_aliases={6: 0},
        compiler_params=pltpu.CompilerParams(vmem_limit_bytes=VMEM_BYTES),
        cost_estimate=pl.CostEstimate(flops=20 * m.size, bytes_accessed=16 * m.size, transcendentals=0),
        name="adamw_of_other",
    )(me, factor, g, w, m, v, out)


def place_kernel(n, at, me_ref, _, *refs):
    pieces, out, turn, bufs, sems = refs[:n], refs[n], refs[n + 1], refs[n + 2 : 2 * n + 2], refs[2 * n + 2]
    turn[0] = me_ref[0]
    loads = [pltpu.make_async_copy(p, b, sems.at[0, k]) for k, (p, b) in enumerate(zip(pieces, bufs))]
    for c in loads:
        c.start()
    stores = []
    for k in range(n):
        loads[k].wait()
        stores.append(pltpu.make_async_copy(bufs[k], out.at[at(k, me_ref[0])], sems.at[1, k]))
        stores[k].start()
    for c in stores:
        c.wait()


def place(out, me, pieces, owners, layer, first, by_columns):
    rows, cols = pieces[0].shape

    def at(k, me):
        owner = me ^ owners[k]
        if by_columns:
            return layer, pl.ds(pl.multiple_of(owner * rows, 8), rows), pl.ds(first * DEVICES * LANES, cols)
        return layer, pl.ds(pl.multiple_of(owner * (out.shape[1] // DEVICES) + first * LANES, LANES), rows), slice(None)

    n = len(pieces)
    return pl.pallas_call(
        functools.partial(place_kernel, n, at),
        in_specs=[pl.BlockSpec(memory_space=pltpu.SMEM)] + [ANY] * (n + 1),
        out_specs=[ANY, pl.BlockSpec(memory_space=pltpu.SMEM)],
        out_shape=[jax.ShapeDtypeStruct(out.shape, out.dtype), jax.ShapeDtypeStruct(me.shape, me.dtype)],
        scratch_shapes=[pltpu.VMEM((rows, cols), BF16)] * n + [pltpu.SemaphoreType.DMA((2, n))],
        input_output_aliases={1: 0},
        compiler_params=pltpu.CompilerParams(vmem_limit_bytes=VMEM_BYTES),
        cost_estimate=pl.CostEstimate(flops=4 * n * rows * cols, bytes_accessed=4 * n * rows * cols, transcendentals=0),
        name="place",
    )(me, out, *pieces)


def other_chip(a):
    return lax.ppermute(a, "dp", [(i, i ^ 2) for i in range(4)])


def other_core(a):
    return lax.ppermute(a, "dp", [(i, i ^ 1) for i in range(4)])


CHUNKS = (
    (0, 0, 0, 1), (0, 0, 1, 3), (0, 0, 4, 5), (0, 1, 0, 9), (1, 0, 0, 9), (1, 1, 0, 9), (2, 0, 0, 9), (2, 1, 3, 3), (2, 1, 6, 2), (2, 1, 8, 1),
)


def solution(mesh):
    def step(x, dy, *arrays):
        weights, m, v = (arrays[i : i + 3] for i in (0, 3, 6))
        me = lax.axis_index("dp").astype(jnp.int32).reshape(1)
        *g, factor, m_other, v_other, g_other = gradients(x[0], dy[0], *weights, m[2], v[2])
        new = [None] * 3
        gathered = []
        for k, layer, first, steps in CHUNKS:
            new[k], sent, me = adamw(me, factor, g[k], weights[k], m[k], v[k], new[k], layer, first, steps, k < 2)
            far = other_chip(sent)
            own = other_core(sent)
            gathered.append((far, own, other_core(far)))
        new[2], sent, me = adamw(me, factor, g[2], weights[2], m[2], v[2], new[2], 1, 0, EARLY, False)
        whole = [n[0] for n in new]
        whole[2], far, me = adamw_of_other(me, factor, g_other, weights[2], m_other, v_other, whole[2], 1)
        own = other_core(sent)
        far = other_core(far)
        whole[2], me = place(whole[2], me, (own, far), (1, 3), 1, 0, False)
        for (k, layer, first, steps), pieces in zip(CHUNKS, gathered):
            whole[k], me = place(whole[k], me, pieces, (2, 1, 3), layer, first, k < 2)
        return (*whole, *(n[1] for n in new), *(n[2] for n in new))

    rows = P(None, "dp", None)
    return jax.shard_map(
        step,
        mesh=mesh,
        in_specs=(P(("rep", "dp")), P(("rep", "dp")), *(P(),) * 3, *(rows,) * 6),
        out_specs=(*(P("rep"),) * 3, *(P("rep", "dp"),) * 6),
        check_vma=False,
    )
```

```python
import functools

import jax
import jax.numpy as jnp
from jax import lax
from jax.experimental import pallas as pl
from jax.experimental.pallas import tpu as pltpu
from jax.sharding import PartitionSpec as P


F32, BF16 = jnp.float32, jnp.bfloat16
DEVICES = 4
LANES = 128
SOME = 32
FACTOR = pl.BlockSpec((8, LANES), lambda i, me: (0, 0))
CHUNK = 256
EARLY = 4
ANY = pl.BlockSpec(memory_space=pl.ANY)
VMEM_BYTES = 67_043_328


def dot(a, b, dims):
    return lax.dot_general(a, b, (dims, ((), ())), preferred_element_type=F32)


NN, NT, TT = ((1,), (0,)), ((1,), (1,)), ((0,), (1,))


def sigmoid(x):
    return 1.0 / (1.0 + jnp.exp(-x))


def loop(n, body):
    lax.fori_loop(0, n, lambda i, c: (body(i), c)[1], 0)


def apart(cond, body):
    lax.fori_loop(0, jnp.where(cond, 1, 0), lambda i, c: (body(), c)[1], 0)


def grads_kernel(
    x, dy, wg, wu, wd, md, vd,
    gg, gu, gd, factor, mo, vo, go, ge, gate_s, up_s, a0t_s, ht_s, mate, own, far, cross,
    DN, A, AT, DD, DT, ACC, GR, ACT, DG, DU, WG, WU, WD, G0, U0, D0, G1, U1, D1, MATEB, FB, SQ, SQS,
    wsem, iosem, d2d_send, d2d_recv, near_recv, free, own_sem, far_sem, x_send, x_recv, fsem, sq_send, sq_recv, e_sem, e_send, e_recv,
):
    T, D = x.shape
    F = wg.shape[2]
    W = DEVICES * LANES
    NT_ = F // W
    BOTH, HALF, PART = 2 * NT_, D // 2, 96
    FAR, NEAR = 0, 1
    H = T // 2
    R = D // DEVICES
    me = lax.axis_index("dp")
    chip, core = me // 2, me % 2
    mate_id, cross_id = {"dp": chip * 2 + 1 - core}, {"dp": (1 - chip) * 2 + core}
    lo, hi = pl.ds(0, H), pl.ds(H, H)

    barrier = pltpu.get_barrier_semaphore()
    for k in range(1, DEVICES):
        pl.semaphore_signal(barrier, inc=1, device_id={"dp": (me + k) % DEVICES}, device_id_type=pl.DeviceIdType.MESH)

    def columns(p, j):
        return pl.ds(pl.multiple_of(p * (F // DEVICES) + j * LANES, LANES), LANES)

    def weights(l, j, q, down_only=False):
        slot = q % 2
        copies = []
        for p in range(DEVICES):
            piece = pl.ds(p * LANES, LANES)
            if not down_only:
                copies.append(pltpu.make_async_copy(wg.at[l, :, columns(p, j)], WG.at[slot, :, piece], wsem.at[slot, 0, p]))
                copies.append(pltpu.make_async_copy(wu.at[l, :, columns(p, j)], WU.at[slot, :, piece], wsem.at[slot, 1, p]))
            copies.append(pltpu.make_async_copy(wd.at[l, columns(p, j), :], WD.at[slot, piece, :], wsem.at[slot, 2, p]))
        return copies

    def start(copies):
        for c in copies:
            c.start()

    def wait(copies):
        for c in copies:
            c.wait()

    def owner_chip(side):
        return 1 - chip if side == FAR else chip

    def d2d(t, side):
        return pltpu.make_async_remote_copy(
            src_ref=GR.at[:, owner_chip(side), 1 - core], dst_ref=MATEB if side == FAR else mate.at[t],
            send_sem=d2d_send.at[side], recv_sem=d2d_recv if side == FAR else near_recv.at[t],
            device_id=mate_id, device_id_type=pl.DeviceIdType.MESH)

    def keep(t):
        return pltpu.make_async_copy(GR.at[:, chip, core], own.at[t], own_sem)

    def across(t, direct=True):
        return pltpu.make_async_remote_copy(
            src_ref=FB.at[t % 2] if direct else far.at[t], dst_ref=cross.at[t], send_sem=x_send.at[t], recv_sem=x_recv.at[t],
            device_id=cross_id, device_id_type=pl.DeviceIdType.MESH)

    def moments():
        rows = pl.ds(0, EARLY * LANES)
        return [
            pltpu.make_async_remote_copy(
                src_ref=src.at[1, rows], dst_ref=dst, send_sem=e_send.at[n], recv_sem=e_recv.at[n],
                device_id=cross_id, device_id_type=pl.DeviceIdType.MESH)
            for n, (src, dst) in enumerate(((md, mo), (vd, vo)))
        ]

    def early_rows(t):
        return pl.ds(pl.multiple_of(t * LANES, LANES), LANES)

    def early_send(t):
        return pltpu.make_async_remote_copy(
            src_ref=ge.at[early_rows(t)], dst_ref=go.at[early_rows(t)], send_sem=e_send.at[2 + t], recv_sem=e_recv.at[2 + t],
            device_id=cross_id, device_id_type=pl.DeviceIdType.MESH)

    def early_store(t):
        return pltpu.make_async_copy(DN, ge.at[early_rows(t)], e_sem.at[3])

    def early_loads(t):
        return [
            pltpu.make_async_copy(src.at[t, 2], D0.at[pl.ds(n * R, R)], e_sem.at[n]) for n, src in enumerate((own, mate, cross))
        ]

    def early_begin(t):
        across(t).wait_recv()
        d2d(t, NEAR).wait_recv()
        start(early_loads(t))

    def early_sum(t):
        wait(early_loads(t))
        g = (D0[0:R, :].astype(F32) + D0[R : 2 * R, :].astype(F32) + D0[2 * R : 3 * R, :].astype(F32)).astype(BF16)
        DN[:] = tall(g).T
        early_store(t).start()

    def tall(g):
        return jnp.concatenate([g[:, q * LANES : (q + 1) * LANES] for q in range(DEVICES)], axis=0)

    def far_store(t):
        return pltpu.make_async_copy(FB.at[t % 2], far.at[t], far_sem)

    def send_far(t):
        pl.when(t > 0)(lambda: pl.semaphore_wait(free, 1))
        d2d(t, FAR).start()

    def far_sum(t):
        d2d(t, FAR).wait_recv()

        def some(i):
            rows = pl.ds(pl.multiple_of(i * PART, PART), PART)
            for k in range(3):
                FB[t % 2, k, rows, :] = (GR[k, 1 - chip, core, rows, :].astype(F32) + MATEB[k, rows, :].astype(F32)).astype(BF16)

        loop(R // PART, some)
        pl.semaphore_signal(free, inc=1, device_id=mate_id, device_id_type=pl.DeviceIdType.MESH)

    def sent(t):
        d2d(t, FAR).wait_send()
        d2d(t, NEAR).wait_send()
        keep(t).wait()

    def put(k, h, value, first=0):
        value = value.astype(BF16)
        for o in range(2):
            if k < 2:
                GR[k, h, o] = value[o * R : (o + 1) * R]
            else:
                for q in range(value.shape[0] // R):
                    lanes = slice((first + q) * LANES, (first + q + 1) * LANES)
                    GR[k, h, o, :, lanes] = value[q * R : (q + 1) * R, o * LANES : (o + 1) * LANES]

    def side_of(i):
        return jnp.where(i == 0, 1 - chip, chip)

    def hidden_of(h):
        return pl.ds(pl.multiple_of(h * (W // 2), W // 2), W // 2)

    def half_of(i):
        return pl.ds(pl.multiple_of(i * HALF, HALF), HALF)

    def product_back(g_ref, u_ref, d_ref, r0):
        step = 16
        for r in range(0, H, step):
            g, u = g_ref(r, step), u_ref(r, step)
            d = d_ref[r : r + step, :].astype(F32)
            s = sigmoid(g)
            si = g * s
            ACT[r0 + r : r0 + r + step, :] = (si * u).astype(BF16)
            DU[r0 + r : r0 + r + step, :] = (d * si).astype(BF16)
            DG[r0 + r : r0 + r + step, :] = (d * u * (s + si * (1.0 - s))).astype(BF16)

    def columns_of(i):
        return pl.ds(pl.multiple_of(i * CHUNK, CHUNK), CHUNK)

    def down_rows(step, body):
        for r in range(0, D, step):
            body(slice(r, r + step))

    def summed(parts):
        return jnp.sum(sum(parts), axis=0, keepdims=True)

    def scale_of(mean_square):
        return lax.rsqrt(mean_square + 1e-6)

    def folded(t):
        return jnp.sum(t.reshape(t.shape[0] // 8, 8, t.shape[1]), axis=0)

    def turn(src, rows, dst):
        for c in range(0, T, 2 * LANES):
            dst[rows, c : c + 2 * LANES] = src[c : c + 2 * LANES, rows].T

    def loads(j):
        return [
            pltpu.make_async_copy(to.at[j, pl.ds(half * H, H), :], ref, iosem.at[3 + 2 * half + n])
            for half, refs in enumerate(((G0, U0), (G1, U1)))
            for n, (ref, to) in enumerate(zip(refs, (gate_s, up_s)))
        ]

    def load_h(HB, i):
        return pltpu.make_async_copy(ht_s.at[i], HB.at[i % 2], iosem.at[1 + i % 2])

    load_a0t = pltpu.make_async_copy(a0t_s, AT, iosem.at[0])

    def norm_back(HB):
        n = T // CHUNK

        def part(i):
            r = columns_of(i)
            slot = i % 2
            load_h(HB, i).wait()

            squares, along = [], []

            def add(rows):
                wide = HB[slot, rows, :].astype(F32)
                squares.append(folded(wide * wide))
                along.append(folded(ACC[rows, r].astype(BF16).astype(F32) * wide))

            down_rows(64, add)
            scale = scale_of(summed(squares) / D)
            shrink = summed(along) / D * (scale * scale * scale)

            def back(rows):
                wide = HB[slot, rows, :].astype(F32)
                dwide = ACC[rows, r].astype(BF16).astype(F32) * scale - wide * shrink
                dh = (DT[rows, r].astype(F32) + dwide.astype(BF16).astype(F32)).astype(BF16)
                DT[rows, r] = dh
                DD[r, rows] = dh.T

            down_rows(LANES, back)
            apart(i < n - 2, lambda: load_h(HB, i + 2).start())

        loop(n, part)
        sent(NT_ - 1)
        load_a0t.start()

    def first_half():
        S = ((G0, U0, D0), (G1, U1, D1))

        def forward(TB):
            load_x = [pltpu.make_async_copy(x.at[pl.ds(c * (T // 4), T // 4)], DD.at[pl.ds(c * (T // 4), T // 4)], iosem.at[c]) for c in range(4)]
            start(load_x)
            start(weights(0, 0, 0))

            def zero(i):
                ACC[pl.ds(pl.multiple_of(i * LANES, LANES), LANES), :] = jnp.zeros((LANES, T), F32)

            loop(D // LANES, zero)

            def norm_x(i):
                r = pl.ds(pl.multiple_of(i * LANES, LANES), LANES)
                wide = DD[r, :].astype(F32)
                A[r, :] = (wide * scale_of(jnp.mean(wide * wide, axis=1, keepdims=True))).astype(BF16)
                AT[:, r] = DD[r, :].T

            for c in range(4):
                load_x[c].wait()
                loop(T // 4 // LANES, lambda i, c=c: norm_x(c * (T // 4 // LANES) + i))
            load_dy = pltpu.make_async_copy(dy, DD, iosem.at[6])
            load_dy.start()
            pl.semaphore_wait(barrier, DEVICES - 1)
            start(moments())

            def stores(j, half):
                return [
                    pltpu.make_async_copy(ref, to.at[j, pl.ds(half * H, H), :], iosem.at[2 * half + n])
                    for n, (ref, to) in enumerate(zip(S[half][:2], (gate_s, up_s)))
                ]

            def save(j):
                return pltpu.make_async_copy(TB.at[j % 2], a0t_s.at[pl.ds(pl.multiple_of(j * LANES, LANES), LANES), :], iosem.at[4 + j % 2])

            def projections(half, slot):
                rows = lo if half == 0 else hi
                S[half][0][:] = dot(A[rows, :], WG[slot], NN)
                S[half][1][:] = dot(A[rows, :], WU[slot], NN)

            def product(half):
                g_ref, u_ref, _ = S[half]
                for r in range(0, H, 16):
                    g = g_ref[r : r + 16, :]
                    ACT[half * H + r : half * H + r + 16, :] = (g * sigmoid(g) * u_ref[r : r + 16, :]).astype(BF16)

            def down(rows, slot):
                ACC[:, rows] += dot(WD[slot], ACT[rows, :], TT)

            def tile(j):
                slot = j % 2
                some = pl.ds(pl.multiple_of(j * LANES, LANES), LANES)
                wait(weights(0, j, j))

                @pl.when(j < NT_ - 1)
                def _():
                    start(weights(0, j + 1, j + 1))

                @pl.when(j == NT_ - 1)
                def _():
                    start(weights(1, 0, NT_))

                @pl.when(j > 0)
                def _():
                    wait(stores(j - 1, 0) + stores(j - 1, 1))

                @pl.when(j > 1)
                def _():
                    save(j - 2).wait()

                projections(0, slot)
                for c in range(0, T, 2 * LANES):
                    TB[slot, :, c : c + 2 * LANES] = A[c : c + 2 * LANES, some].T
                start(stores(j, 0))
                save(j).start()
                projections(1, slot)
                product(0)
                start(stores(j, 1))

                @pl.when(j == 0)
                def _():
                    load_dy.wait()

                down(lo, slot)
                product(1)
                turn(DD, some, DT)
                down(hi, slot)

            loop(NT_, tile)
            wait(stores(NT_ - 1, 0) + stores(NT_ - 1, 1))
            save(NT_ - 2).wait()
            save(NT_ - 1).wait()

        pl.run_scoped(forward, pltpu.VMEM((2, LANES, T), BF16))

        def norm_h(HB):
            n = T // CHUNK

            def save(i):
                return pltpu.make_async_copy(HB.at[i % 2], ht_s.at[i], iosem.at[i % 2])

            def part(i):
                r = columns_of(i)
                slot = i % 2

                @pl.when(i > 1)
                def _():
                    save(i - 2).wait()

                squares = []

                def add(rows):
                    h = (AT[rows, r].astype(F32) + ACC[rows, r].astype(BF16).astype(F32)).astype(BF16)
                    HB[slot, rows, :] = h
                    ACC[rows, r] = jnp.zeros((h.shape[0], CHUNK), F32)
                    wide = h.astype(F32)
                    squares.append(folded(wide * wide))

                down_rows(64, add)
                save(i).start()
                scale = scale_of(summed(squares) / D)

                def norm(rows):
                    a = (HB[slot, rows, :].astype(F32) * scale).astype(BF16)
                    AT[rows, r] = a
                    A[r, rows] = a.T

                down_rows(LANES, norm)

            loop(n, part)
            save(n - 2).wait()
            save(n - 1).wait()

        pl.run_scoped(norm_h, pltpu.VMEM((2, D, CHUNK), BF16))

        def layer1(HB):
            def projections(half, slot):
                rows = lo if half == 0 else hi
                S[half][0][:] = dot(A[rows, :], WG[slot], NN)
                S[half][1][:] = dot(A[rows, :], WU[slot], NN)
                S[half][2][:] = dot(DD[rows, :], WD[slot], NT).astype(BF16)

            def back(half):
                g_ref, u_ref, d_ref = S[half]
                product_back(lambda r, n: g_ref[r : r + n, :], lambda r, n: u_ref[r : r + n, :], d_ref, half * H)

            def da(rows, slot):
                ACC[:, rows] += dot(WG[slot], DG[rows, :], NT)
                ACC[:, rows] += dot(WU[slot], DU[rows, :], NT)

            def tile(j):
                slot = (NT_ + j) % 2
                wait(weights(1, j, NT_ + j))

                @pl.when(j < NT_ - 1)
                def _():
                    start(weights(1, j + 1, NT_ + j + 1))

                @pl.when(j == NT_ - 1)
                def _():
                    start(weights(0, 0, BOTH, True))

                projections(0, slot)
                projections(1, slot)
                back(0)
                apart(j > 0, lambda: sent(j - 1))
                apart((j > 2) & (j < 3 + EARLY), lambda: early_store(j - 3).wait())
                apart((j > 2) & (j < 2 + EARLY), lambda: early_send(j - 3).start())
                apart((j > 1) & (j < 2 + EARLY), lambda: early_begin(j - 2))
                da(lo, slot)
                back(1)
                da(hi, slot)
                apart(j == NT_ - 1, lambda: start([load_h(HB, 0), load_h(HB, 1), *loads(0)]))

                def gradients(i):
                    h = side_of(i)
                    for q in (0, 2):
                        put(2, h, dot(DT[q * R : (q + 2) * R, :], ACT[:, hidden_of(h)], NN), q)
                    for k, rhs in ((0, DG), (1, DU)):
                        put(k, h, dot(AT[half_of(h), :], rhs[:], NN))
                    apart(i == 0, lambda: send_far(j))

                loop(2, gradients)
                d2d(j, NEAR).start()
                keep(j).start()
                apart(j > 1, lambda: across(j - 2).wait_send())
                far_sum(j)
                across(j).start()
                apart((j > 1) & (j < 2 + EARLY), lambda: early_sum(j - 2))

            loop(NT_, tile)
            norm_back(HB)

        pl.run_scoped(layer1, pltpu.VMEM((2, D, CHUNK), BF16))

    first_half()

    def layer0():
        S = ((G0, U0, D0), (G1, U1, D1))

        def tile(j):
            t = NT_ + j
            slot = j % 2
            half_sum = pl.ds(0, W)

            def back(half):
                g_ref, u_ref, d_ref = S[half]
                product_back(lambda r, n: g_ref[r : r + n, :], lambda r, n: u_ref[r : r + n, :], d_ref, half * H)

            wait(weights(0, j, BOTH + j, True))

            @pl.when(j < NT_ - 1)
            def _():
                start(weights(0, j + 1, BOTH + j + 1, True))

            wait(loads(j))
            D0[:] = dot(DD[lo, :], WD[slot], NT).astype(BF16)
            D1[:] = dot(DD[hi, :], WD[slot], NT).astype(BF16)
            back(0)
            ACC[:, half_sum] = dot(DT[:, lo], ACT[lo, :], NN)
            back(1)
            apart(j < NT_ - 1, lambda: start(loads(j + 1)))
            apart(j == 0, lambda: load_a0t.wait())
            apart(j > 0, lambda: sent(t - 1))

            def gradients(i):
                h = side_of(i)
                for q in (0, 2):
                    rows = slice(q * R, (q + 2) * R)
                    put(2, h, ACC[rows, hidden_of(h)] + dot(DT[rows, hi], ACT[hi, hidden_of(h)], NN), q)
                for k, rhs in ((0, DG), (1, DU)):
                    put(k, h, dot(AT[half_of(h), :], rhs[:], NN))
                apart((j > 1) & (i == 0), lambda: (far_store(t - 1).wait(), across(t - 1, False).start()))
                apart(i == 0, lambda: send_far(t))

            loop(2, gradients)
            d2d(t, NEAR).start()
            keep(t).start()
            apart(j < 3, lambda: across(t - 2).wait_send())
            far_sum(t)
            apart(j == 0, lambda: across(t).start())
            apart(j > 0, lambda: far_store(t).start())

        loop(NT_, tile)

    layer0()

    last = BOTH - 1
    far_store(last).wait()
    across(last, False).start()
    early_send(EARLY - 1).start()
    sent(last)
    pl.semaphore_wait(free, 1)

    def finish():
        GN, UN, CB = GR.at[0, 1, 0], GR.at[0, 1, 1], GR.at[:, 0, 0]
        SQ[:] = jnp.zeros_like(SQ)

        def outs(t):
            l, j = 1 - t // NT_, t % NT_
            copies = []
            for p in range(DEVICES):
                copies.append(pltpu.make_async_copy(GN.at[:, pl.ds(p * LANES, LANES)], gg.at[l, :, columns(p, j)], fsem.at[3 + p]))
                copies.append(pltpu.make_async_copy(UN.at[:, pl.ds(p * LANES, LANES)], gu.at[l, :, columns(p, j)], fsem.at[7 + p]))
            rows = pl.ds(pl.multiple_of(j * LANES, LANES), LANES)
            copies.append(pltpu.make_async_copy(DN, gd.at[l, rows, :], fsem.at[11]))
            return copies

        def one(t):
            ins = [
                pltpu.make_async_copy(own.at[t], FB.at[0], fsem.at[0]),
                pltpu.make_async_copy(mate.at[t], FB.at[1], fsem.at[1]),
                pltpu.make_async_copy(cross.at[t], CB, fsem.at[2]),
            ]
            apart(t >= EARLY, lambda: d2d(t, NEAR).wait_recv())
            start(ins[:2])
            apart(t >= EARLY, lambda: across(t, False).wait_recv())
            ins[2].start()
            apart(t > NT_, lambda: across(t, False).wait_send())

            @pl.when(t > 0)
            def _():
                wait(outs(t - 1))

            wait(ins)
            for k in range(3):
                total = FB[0, k].astype(F32) + FB[1, k].astype(F32) + CB[k].astype(F32)
                g = total.astype(BF16)
                wide = g.astype(F32)
                SQ[:] += jnp.sum((wide * wide).reshape(R // 8, 8, W), axis=0)
                if k == 0:
                    GN[:] = g
                elif k == 1:
                    UN[:] = g
                else:
                    DN[:] = tall(g).T
            start(outs(t))

        loop(BOTH, one)

        mine = jnp.sum(SQ[:], keepdims=True)
        SQS[DEVICES] = jnp.broadcast_to(mine, (8, LANES))
        copies = [
            pltpu.make_async_remote_copy(
                src_ref=SQS.at[DEVICES], dst_ref=SQS.at[me], send_sem=sq_send.at[k - 1], recv_sem=sq_recv.at[k - 1],
                device_id={"dp": (me + k) % DEVICES}, device_id_type=pl.DeviceIdType.MESH)
            for k in range(1, DEVICES)
        ]
        start(copies)
        SQS[me] = jnp.broadcast_to(mine, (8, LANES))
        wait(outs(last))
        for k in range(1, DEVICES):
            came = SQS.at[(me + DEVICES - k) % DEVICES]
            pltpu.make_async_copy(came, came, sq_recv.at[k - 1]).wait()
            copies[k - 1].wait_send()

    finish()
    for c in moments():
        c.wait()
    for t in range(EARLY):
        early_send(t).wait()

    total = sum(SQS[k] for k in range(DEVICES))
    count = 2.0 * 3.0 * D * F
    factor[:] = jnp.minimum(1.0, 0.5 * lax.rsqrt(total / count + 1e-30))


def gradients(x, dy, wg, wu, wd, md, vd):
    T, D = x.shape
    F = wg.shape[2]
    W = DEVICES * LANES
    n, R = F // W, D // DEVICES
    tiles = 2 * n
    hbm = lambda *s, d=BF16: jax.ShapeDtypeStruct(s, d)
    outs = [
        hbm(2, R, F), hbm(2, R, F), hbm(2, F // DEVICES, D), hbm(8, LANES, d=F32),
        hbm(EARLY * LANES, D, d=F32), hbm(EARLY * LANES, D, d=F32), hbm(EARLY * LANES, D), hbm(EARLY * LANES, D),
        hbm(n, T, W, d=F32), hbm(n, T, W, d=F32), hbm(D, T), hbm(T // CHUNK, D, CHUNK),
        hbm(tiles, 3, R, W), hbm(tiles, 3, R, W), hbm(tiles, 3, R, W), hbm(tiles, 3, R, W),
    ]
    sem = pltpu.SemaphoreType.DMA
    return pl.pallas_call(
        grads_kernel,
        out_shape=outs,
        in_specs=[ANY] * 7,
        out_specs=[ANY] * 3 + [pl.BlockSpec(memory_space=pltpu.VMEM)] + [ANY] * 12,
        scratch_shapes=[
            pltpu.VMEM((LANES, D), BF16),
            pltpu.VMEM((T, D), BF16), pltpu.VMEM((D, T), BF16), pltpu.VMEM((T, D), BF16), pltpu.VMEM((D, T), BF16),
            pltpu.VMEM((D, T), F32), pltpu.VMEM((3, 2, 2, R, W), BF16), *[pltpu.VMEM((T, W), BF16)] * 3,
            pltpu.VMEM((2, D, W), BF16), pltpu.VMEM((2, D, W), BF16), pltpu.VMEM((2, W, D), BF16),
            *[pltpu.VMEM((T // 2, W), F32), pltpu.VMEM((T // 2, W), F32), pltpu.VMEM((T // 2, W), BF16)] * 2,
            pltpu.VMEM((3, R, W), BF16), pltpu.VMEM((2, 3, R, W), BF16),
            pltpu.VMEM((8, W), F32), pltpu.VMEM((DEVICES + 1, 8, LANES), F32),
            sem((2, 3, DEVICES)), sem((7,)), sem((2,)), sem(()), sem((tiles,)), pltpu.SemaphoreType.REGULAR, sem(()), sem(()),
            sem((tiles,)), sem((tiles,)), sem((12,)), sem((DEVICES - 1,)), sem((DEVICES - 1,)),
            sem((4,)), sem((2 + EARLY,)), sem((2 + EARLY,)),
        ],
        compiler_params=pltpu.CompilerParams(collective_id=0, has_side_effects=True, vmem_limit_bytes=VMEM_BYTES),
        name="gradients",
    )(x, dy, wg, wu, wd, md, vd)[:7]


def cost(n):
    return pl.CostEstimate(flops=4 * n, bytes_accessed=4 * n, transcendentals=0)


def stepped(factor, g, w, m, v):
    grad = g.astype(F32) * factor[:1, :1]
    m = 0.9 * m + 0.1 * grad
    v = 0.95 * v + 0.05 * grad * grad
    wide = w.astype(F32)
    return (wide - 0.02 * (m * lax.rsqrt(v + 1e-8) + 0.1 * wide)).astype(BF16), m, v


def adamw_kernel(me, factor, g, w, m, v, *refs):
    out, send, new_m, new_v, turn = refs[-5:]
    turn[0] = me[0]

    def part(i):
        r = pl.ds(pl.multiple_of(i * SOME, SOME), SOME)
        out[r, :], new_m[r, :], new_v[r, :] = stepped(factor, g[r, :], w[r, :], m[r, :], v[r, :])
        send[r, :] = out[r, :]

    loop(m.shape[0] // SOME, part)


def adamw(me, factor, g, w, m, v, so_far, layer, first, steps, by_columns):
    rows = m.shape[1] if by_columns else LANES
    cols = DEVICES * LANES if by_columns else m.shape[2]
    tile = (None, rows, cols)
    if by_columns:
        block = pl.BlockSpec(tile, lambda i, me: (layer, 0, first + i))
        whole = pl.BlockSpec(tile, lambda i, me: (layer, me[0], first + i))
        alone, send = (rows, steps * cols), pl.BlockSpec((rows, cols), lambda i, me: (0, i))
    else:
        n = m.shape[1] // LANES
        block = pl.BlockSpec(tile, lambda i, me: (layer, first + i, 0))
        whole = pl.BlockSpec(tile, lambda i, me: (layer, me[0] * n + first + i, 0))
        alone, send = (steps * rows, cols), pl.BlockSpec((rows, cols), lambda i, me: (i, 0))
    begun = so_far is not None
    shape = lambda a: jax.ShapeDtypeStruct(a.shape, a.dtype)
    out, sent, new_m, new_v, turn = pl.pallas_call(
        adamw_kernel,
        grid_spec=pltpu.PrefetchScalarGridSpec(
            num_scalar_prefetch=1,
            grid=(steps,),
            in_specs=[FACTOR, block, whole, block, block] + [ANY] * (3 * begun),
            out_specs=[whole, send, block, block, pl.BlockSpec(memory_space=pltpu.SMEM)],
        ),
        out_shape=[shape(w), jax.ShapeDtypeStruct(alone, BF16), shape(m), shape(v), shape(me)],
        input_output_aliases={6: 0, 7: 2, 8: 3} if begun else {},
        compiler_params=pltpu.CompilerParams(vmem_limit_bytes=VMEM_BYTES),
        cost_estimate=cost(5 * steps * rows * cols),
        name="adamw",
    )(me, factor, g, w, m, v, *(so_far or ()))
    return (out, new_m, new_v), sent, turn


def other_kernel(me, factor, g, w, m, v, _, out, send, turn):
    turn[0] = me[0]
    out[:], *_ = stepped(factor, g[:], w[:], m[:], v[:])
    send[:] = out[:]


def adamw_of_other(me, factor, g, w, m, v, out, layer):
    D = m.shape[1]
    n = w.shape[1] // DEVICES // LANES
    block = pl.BlockSpec((LANES, D), lambda i, me: (i, 0))
    whole = pl.BlockSpec((None, LANES, D), lambda i, me: (layer, (me[0] ^ 2) * n + i, 0))
    return pl.pallas_call(
        other_kernel,
        grid_spec=pltpu.PrefetchScalarGridSpec(
            num_scalar_prefetch=1,
            grid=(EARLY,),
            in_specs=[FACTOR, block, whole, block, block, ANY],
            out_specs=[whole, block, pl.BlockSpec(memory_space=pltpu.SMEM)],
        ),
        out_shape=[jax.ShapeDtypeStruct(w.shape, BF16), jax.ShapeDtypeStruct(m.shape, BF16), jax.ShapeDtypeStruct(me.shape, me.dtype)],
        input_output_aliases={6: 0},
        compiler_params=pltpu.CompilerParams(vmem_limit_bytes=VMEM_BYTES),
        cost_estimate=cost(m.size),
        name="adamw_of_other",
    )(me, factor, g, w, m, v, out)


def place_kernel(n, at, me_ref, _, *refs):
    pieces, out, turn, bufs, sems = refs[:n], refs[n], refs[n + 1], refs[n + 2 : 2 * n + 2], refs[2 * n + 2]
    turn[0] = me_ref[0]
    loads = [pltpu.make_async_copy(p, b, sems.at[0, k]) for k, (p, b) in enumerate(zip(pieces, bufs))]
    for c in loads:
        c.start()
    stores = []
    for k in range(n):
        loads[k].wait()
        stores.append(pltpu.make_async_copy(bufs[k], out.at[at(k, me_ref[0])], sems.at[1, k]))
        stores[k].start()
    for c in stores:
        c.wait()


def place(out, me, pieces, owners, layer, first, by_columns):
    rows, cols = pieces[0].shape

    def at(k, me):
        owner = me ^ owners[k]
        if by_columns:
            return layer, pl.ds(pl.multiple_of(owner * rows, 8), rows), pl.ds(first * DEVICES * LANES, cols)
        return layer, pl.ds(pl.multiple_of(owner * (out.shape[1] // DEVICES) + first * LANES, LANES), rows), slice(None)

    n = len(pieces)
    return pl.pallas_call(
        functools.partial(place_kernel, n, at),
        in_specs=[pl.BlockSpec(memory_space=pltpu.SMEM)] + [ANY] * (n + 1),
        out_specs=[ANY, pl.BlockSpec(memory_space=pltpu.SMEM)],
        out_shape=[jax.ShapeDtypeStruct(out.shape, out.dtype), jax.ShapeDtypeStruct(me.shape, me.dtype)],
        scratch_shapes=[pltpu.VMEM((rows, cols), BF16)] * n + [pltpu.SemaphoreType.DMA((2, n))],
        input_output_aliases={1: 0},
        compiler_params=pltpu.CompilerParams(vmem_limit_bytes=VMEM_BYTES),
        cost_estimate=cost(n * rows * cols),
        name="place",
    )(me, out, *pieces)


def other_chip(a):
    return lax.ppermute(a, "dp", [(i, i ^ 2) for i in range(4)])


def other_core(a):
    return lax.ppermute(a, "dp", [(i, i ^ 1) for i in range(4)])


ORDER = ((0, 0, (1, 2, 6)), (0, 1, (9,)), (1, 0, (9,)), (1, 1, (9,)), (2, 0, (9,)), (2, 1, (2, 2, 1)))


def chunks():
    listed = []
    for k, layer, sizes in ORDER:
        first = EARLY if (k, layer) == ORDER[-1][:2] else 0
        for n in sizes:
            listed.append((k, layer, first, n))
            first += n
    return listed


CHUNKS = chunks()


def solution(mesh):
    def step(x, dy, *arrays):
        weights, m, v = (arrays[i : i + 3] for i in (0, 3, 6))
        me = lax.axis_index("dp").astype(jnp.int32).reshape(1)
        *g, factor, m_other, v_other, g_other = gradients(x[0], dy[0], *weights, m[2], v[2])
        new = [None] * 3
        gathered = []
        for k, layer, first, steps in CHUNKS:
            new[k], sent, me = adamw(me, factor, g[k], weights[k], m[k], v[k], new[k], layer, first, steps, k < 2)
            far = other_chip(sent)
            own = other_core(sent)
            gathered.append((far, own, other_core(far)))
        new[2], sent, me = adamw(me, factor, g[2], weights[2], m[2], v[2], new[2], 1, 0, EARLY, False)
        whole = [n[0] for n in new]
        whole[2], far, me = adamw_of_other(me, factor, g_other, weights[2], m_other, v_other, whole[2], 1)
        own = other_core(sent)
        far = other_core(far)
        whole[2], me = place(whole[2], me, (own, far), (1, 3), 1, 0, False)
        for (k, layer, first, steps), pieces in zip(CHUNKS, gathered):
            whole[k], me = place(whole[k], me, pieces, (2, 1, 3), layer, first, k < 2)
        return (*whole, *(n[1] for n in new), *(n[2] for n in new))

    rows = P(None, "dp", None)
    return jax.shard_map(
        step,
        mesh=mesh,
        in_specs=(P(("rep", "dp")), P(("rep", "dp")), *(P(),) * 3, *(rows,) * 6),
        out_specs=(*(P("rep"),) * 3, *(P("rep", "dp"),) * 6),
        check_vma=False,
    )
```

```python
import functools

import jax
import jax.numpy as jnp
from jax import lax
from jax.experimental import pallas as pl
from jax.experimental.pallas import tpu as pltpu
from jax.sharding import PartitionSpec as P


F32, BF16 = jnp.float32, jnp.bfloat16
DEVICES = 4
LANES = 128
SOME = 32
FACTOR = pl.BlockSpec((8, LANES), lambda i, me: (0, 0))
CHUNK = 256
EARLY = 4
ANY = pl.BlockSpec(memory_space=pl.ANY)
VMEM_BYTES = 67_043_328


def dot(a, b, dims):
    return lax.dot_general(a, b, (dims, ((), ())), preferred_element_type=F32)


NN, NT, TT = ((1,), (0,)), ((1,), (1,)), ((0,), (1,))


def sigmoid(x):
    return 1.0 / (1.0 + jnp.exp(-x))


def loop(n, body):
    lax.fori_loop(0, n, lambda i, c: (body(i), c)[1], 0)


def apart(cond, body):
    lax.fori_loop(0, jnp.where(cond, 1, 0), lambda i, c: (body(), c)[1], 0)


def grads_kernel(
    x, dy, wg, wu, wd, md, vd,
    gg, gu, gd, factor, mo, vo, go, ge, gate_s, up_s, a0t_s, ht_s, mate, own, far, cross,
    DN, A, AT, DD, DT, ACC, GR, ACT, DG, DU, WG, WU, WD, G0, U0, D0, G1, U1, D1, MATEB, FB, SQ, SQS,
    wsem, iosem, d2d_send, d2d_recv, near_recv, free, own_sem, far_sem, x_send, x_recv, fsem, sq_send, sq_recv, e_sem, e_send, e_recv,
):
    T, D = x.shape
    F = wg.shape[2]
    W = DEVICES * LANES
    NT_ = F // W
    BOTH, HALF, PART = 2 * NT_, D // 2, 96
    FAR, NEAR = 0, 1
    H = T // 2
    R = D // DEVICES
    me = lax.axis_index("dp")
    chip, core = me // 2, me % 2
    mate_id, cross_id = {"dp": chip * 2 + 1 - core}, {"dp": (1 - chip) * 2 + core}
    lo, hi = pl.ds(0, H), pl.ds(H, H)

    barrier = pltpu.get_barrier_semaphore()
    for k in range(1, DEVICES):
        pl.semaphore_signal(barrier, inc=1, device_id={"dp": (me + k) % DEVICES}, device_id_type=pl.DeviceIdType.MESH)

    def columns(p, j):
        return pl.ds(pl.multiple_of(p * (F // DEVICES) + j * LANES, LANES), LANES)

    def weights(l, j, q, down_only=False):
        slot = q % 2
        copies = []
        for p in range(DEVICES):
            piece = pl.ds(p * LANES, LANES)
            if not down_only:
                copies.append(pltpu.make_async_copy(wg.at[l, :, columns(p, j)], WG.at[slot, :, piece], wsem.at[slot, 0, p]))
                copies.append(pltpu.make_async_copy(wu.at[l, :, columns(p, j)], WU.at[slot, :, piece], wsem.at[slot, 1, p]))
            copies.append(pltpu.make_async_copy(wd.at[l, columns(p, j), :], WD.at[slot, piece, :], wsem.at[slot, 2, p]))
        return copies

    def start(copies):
        for c in copies:
            c.start()

    def wait(copies):
        for c in copies:
            c.wait()

    def owner_chip(side):
        return 1 - chip if side == FAR else chip

    def d2d(t, side):
        return pltpu.make_async_remote_copy(
            src_ref=GR.at[:, owner_chip(side), 1 - core], dst_ref=MATEB if side == FAR else mate.at[t],
            send_sem=d2d_send.at[side], recv_sem=d2d_recv if side == FAR else near_recv.at[t],
            device_id=mate_id, device_id_type=pl.DeviceIdType.MESH)

    def keep(t):
        return pltpu.make_async_copy(GR.at[:, chip, core], own.at[t], own_sem)

    def across(t, direct=True):
        return pltpu.make_async_remote_copy(
            src_ref=FB.at[t % 2] if direct else far.at[t], dst_ref=cross.at[t], send_sem=x_send.at[t], recv_sem=x_recv.at[t],
            device_id=cross_id, device_id_type=pl.DeviceIdType.MESH)

    def moments():
        rows = pl.ds(0, EARLY * LANES)
        return [
            pltpu.make_async_remote_copy(
                src_ref=src.at[1, rows], dst_ref=dst, send_sem=e_send.at[n], recv_sem=e_recv.at[n],
                device_id=cross_id, device_id_type=pl.DeviceIdType.MESH)
            for n, (src, dst) in enumerate(((md, mo), (vd, vo)))
        ]

    def early_rows(t):
        return pl.ds(pl.multiple_of(t * LANES, LANES), LANES)

    def early_send(t):
        return pltpu.make_async_remote_copy(
            src_ref=ge.at[early_rows(t)], dst_ref=go.at[early_rows(t)], send_sem=e_send.at[2 + t], recv_sem=e_recv.at[2 + t],
            device_id=cross_id, device_id_type=pl.DeviceIdType.MESH)

    def early_store(t):
        return pltpu.make_async_copy(DN, ge.at[early_rows(t)], e_sem.at[3])

    def early_loads(t):
        return [
            pltpu.make_async_copy(src.at[t, 2], D0.at[pl.ds(n * R, R)], e_sem.at[n]) for n, src in enumerate((own, mate, cross))
        ]

    def early_begin(t):
        across(t).wait_recv()
        d2d(t, NEAR).wait_recv()
        start(early_loads(t))

    def early_sum(t):
        wait(early_loads(t))
        g = (D0[0:R, :].astype(F32) + D0[R : 2 * R, :].astype(F32) + D0[2 * R : 3 * R, :].astype(F32)).astype(BF16)
        DN[:] = tall(g).T
        early_store(t).start()

    def tall(g):
        return jnp.concatenate([g[:, q * LANES : (q + 1) * LANES] for q in range(DEVICES)], axis=0)

    def far_store(t):
        return pltpu.make_async_copy(FB.at[t % 2], far.at[t], far_sem)

    def send_far(t):
        pl.when(t > 0)(lambda: pl.semaphore_wait(free, 1))
        d2d(t, FAR).start()

    def far_sum(t):
        d2d(t, FAR).wait_recv()

        def some(i):
            rows = pl.ds(pl.multiple_of(i * PART, PART), PART)
            for k in range(3):
                FB[t % 2, k, rows, :] = (GR[k, 1 - chip, core, rows, :].astype(F32) + MATEB[k, rows, :].astype(F32)).astype(BF16)

        loop(R // PART, some)
        pl.semaphore_signal(free, inc=1, device_id=mate_id, device_id_type=pl.DeviceIdType.MESH)

    def sent(t):
        d2d(t, FAR).wait_send()
        d2d(t, NEAR).wait_send()
        keep(t).wait()

    def put(k, h, value, first=0):
        value = value.astype(BF16)
        for o in range(2):
            if k < 2:
                GR[k, h, o] = value[o * R : (o + 1) * R]
            else:
                for q in range(value.shape[0] // R):
                    lanes = slice((first + q) * LANES, (first + q + 1) * LANES)
                    GR[k, h, o, :, lanes] = value[q * R : (q + 1) * R, o * LANES : (o + 1) * LANES]

    def side_of(i):
        return jnp.where(i == 0, 1 - chip, chip)

    def hidden_of(h):
        return pl.ds(pl.multiple_of(h * (W // 2), W // 2), W // 2)

    def half_of(i):
        return pl.ds(pl.multiple_of(i * HALF, HALF), HALF)

    def product_back(g_ref, u_ref, d_ref, r0):
        step = 16
        for r in range(0, H, step):
            g, u = g_ref(r, step), u_ref(r, step)
            d = d_ref[r : r + step, :].astype(F32)
            s = sigmoid(g)
            si = g * s
            ACT[r0 + r : r0 + r + step, :] = (si * u).astype(BF16)
            DU[r0 + r : r0 + r + step, :] = (d * si).astype(BF16)
            DG[r0 + r : r0 + r + step, :] = (d * u * (s + si * (1.0 - s))).astype(BF16)

    def columns_of(i):
        return pl.ds(pl.multiple_of(i * CHUNK, CHUNK), CHUNK)

    def down_rows(step, body):
        for r in range(0, D, step):
            body(slice(r, r + step))

    def summed(parts):
        return jnp.sum(sum(parts), axis=0, keepdims=True)

    def scale_of(mean_square):
        return lax.rsqrt(mean_square + 1e-6)

    def folded(t):
        return jnp.sum(t.reshape(t.shape[0] // 8, 8, t.shape[1]), axis=0)

    def turn(src, rows, dst):
        for c in range(0, T, 2 * LANES):
            dst[rows, c : c + 2 * LANES] = src[c : c + 2 * LANES, rows].T

    def loads(j):
        return [
            pltpu.make_async_copy(to.at[j, pl.ds(half * H, H), :], ref, iosem.at[3 + 2 * half + n])
            for half, refs in enumerate(((G0, U0), (G1, U1)))
            for n, (ref, to) in enumerate(zip(refs, (gate_s, up_s)))
        ]

    def load_h(HB, i):
        return pltpu.make_async_copy(ht_s.at[i], HB.at[i % 2], iosem.at[1 + i % 2])

    load_a0t = pltpu.make_async_copy(a0t_s, AT, iosem.at[0])

    def norm_back(HB):
        n = T // CHUNK

        def part(i):
            r = columns_of(i)
            slot = i % 2
            load_h(HB, i).wait()

            squares, along = [], []

            def add(rows):
                wide = HB[slot, rows, :].astype(F32)
                squares.append(folded(wide * wide))
                along.append(folded(ACC[rows, r].astype(BF16).astype(F32) * wide))

            down_rows(64, add)
            scale = scale_of(summed(squares) / D)
            shrink = summed(along) / D * (scale * scale * scale)

            def back(rows):
                wide = HB[slot, rows, :].astype(F32)
                dwide = ACC[rows, r].astype(BF16).astype(F32) * scale - wide * shrink
                dh = (DT[rows, r].astype(F32) + dwide.astype(BF16).astype(F32)).astype(BF16)
                DT[rows, r] = dh
                DD[r, rows] = dh.T

            down_rows(LANES, back)
            apart(i < n - 2, lambda: load_h(HB, i + 2).start())

        loop(n, part)
        sent(NT_ - 1)
        load_a0t.start()

    def first_half():
        S = ((G0, U0, D0), (G1, U1, D1))

        def forward(TB):
            load_x = [pltpu.make_async_copy(x.at[pl.ds(c * (T // 4), T // 4)], DD.at[pl.ds(c * (T // 4), T // 4)], iosem.at[c]) for c in range(4)]
            start(load_x)
            start(weights(0, 0, 0))

            def zero(i):
                ACC[pl.ds(pl.multiple_of(i * LANES, LANES), LANES), :] = jnp.zeros((LANES, T), F32)

            loop(D // LANES, zero)

            def norm_x(i):
                for n in range(2):
                    r = pl.ds(pl.multiple_of(i * CHUNK + n * LANES, LANES), LANES)
                    wide = DD[r, :].astype(F32)
                    A[r, :] = (wide * scale_of(jnp.mean(wide * wide, axis=1, keepdims=True))).astype(BF16)

            quarter = T // 4 // CHUNK
            for c, load in enumerate(load_x):
                load.wait()
                loop(quarter, lambda i, c=c: norm_x(c * quarter + i))
            load_dy = pltpu.make_async_copy(dy, DD, iosem.at[6])
            pl.semaphore_wait(barrier, DEVICES - 1)
            start(moments())

            def stores(j, half):
                return [
                    pltpu.make_async_copy(ref, to.at[j, pl.ds(half * H, H), :], iosem.at[2 * half + n])
                    for n, (ref, to) in enumerate(zip(S[half][:2], (gate_s, up_s)))
                ]

            def save(j):
                return pltpu.make_async_copy(TB.at[j % 2], a0t_s.at[pl.ds(pl.multiple_of(j * LANES, LANES), LANES), :], iosem.at[4 + j % 2])

            def projections(half, slot):
                rows = lo if half == 0 else hi
                S[half][0][:] = dot(A[rows, :], WG[slot], NN)
                S[half][1][:] = dot(A[rows, :], WU[slot], NN)

            def product(half):
                g_ref, u_ref, _ = S[half]
                for r in range(0, H, 16):
                    g = g_ref[r : r + 16, :]
                    ACT[half * H + r : half * H + r + 16, :] = (g * sigmoid(g) * u_ref[r : r + 16, :]).astype(BF16)

            def down(rows, slot):
                ACC[:, rows] += dot(WD[slot], ACT[rows, :], TT)

            def tile(j):
                slot = j % 2
                some = pl.ds(pl.multiple_of(j * LANES, LANES), LANES)
                wait(weights(0, j, j))

                @pl.when(j < NT_ - 1)
                def _():
                    start(weights(0, j + 1, j + 1))

                @pl.when(j == NT_ - 1)
                def _():
                    start(weights(1, 0, NT_))

                @pl.when(j > 0)
                def _():
                    wait(stores(j - 1, 0) + stores(j - 1, 1))

                @pl.when(j > 1)
                def _():
                    save(j - 2).wait()

                projections(0, slot)
                for c in range(0, T, 2 * LANES):
                    TB[slot, :, c : c + 2 * LANES] = A[c : c + 2 * LANES, some].T
                start(stores(j, 0))
                save(j).start()
                projections(1, slot)
                product(0)
                turn(DD, some, AT)
                start(stores(j, 1))
                apart(j == NT_ - 1, load_dy.start)
                down(lo, slot)
                product(1)
                down(hi, slot)

            loop(NT_, tile)
            wait(stores(NT_ - 1, 0) + stores(NT_ - 1, 1))
            save(NT_ - 2).wait()
            save(NT_ - 1).wait()
            load_dy.wait()

        pl.run_scoped(forward, pltpu.VMEM((2, LANES, T), BF16))

        def norm_h(HB):
            n = T // CHUNK

            def save(i):
                return pltpu.make_async_copy(HB.at[i % 2], ht_s.at[i], iosem.at[i % 2])

            def part(i):
                r = columns_of(i)
                slot = i % 2

                @pl.when(i > 1)
                def _():
                    save(i - 2).wait()

                squares = []

                def add(rows):
                    h = (AT[rows, r].astype(F32) + ACC[rows, r].astype(BF16).astype(F32)).astype(BF16)
                    HB[slot, rows, :] = h
                    ACC[rows, r] = jnp.zeros((h.shape[0], CHUNK), F32)
                    wide = h.astype(F32)
                    squares.append(folded(wide * wide))

                down_rows(64, add)
                save(i).start()
                for q in range(D // LANES):
                    rows = slice(q * LANES, (q + 1) * LANES)
                    DT[rows, r] = DD[r, rows].T
                scale = scale_of(summed(squares) / D)

                def norm(rows):
                    a = (HB[slot, rows, :].astype(F32) * scale).astype(BF16)
                    AT[rows, r] = a
                    A[r, rows] = a.T

                down_rows(LANES, norm)

            loop(n, part)
            save(n - 2).wait()
            save(n - 1).wait()

        pl.run_scoped(norm_h, pltpu.VMEM((2, D, CHUNK), BF16))

        def layer1(HB):
            def projections(half, slot):
                rows = lo if half == 0 else hi
                S[half][0][:] = dot(A[rows, :], WG[slot], NN)
                S[half][1][:] = dot(A[rows, :], WU[slot], NN)
                S[half][2][:] = dot(DD[rows, :], WD[slot], NT).astype(BF16)

            def back(half):
                g_ref, u_ref, d_ref = S[half]
                product_back(lambda r, n: g_ref[r : r + n, :], lambda r, n: u_ref[r : r + n, :], d_ref, half * H)

            def da(rows, slot):
                ACC[:, rows] += dot(WG[slot], DG[rows, :], NT)
                ACC[:, rows] += dot(WU[slot], DU[rows, :], NT)

            def tile(j):
                slot = (NT_ + j) % 2
                wait(weights(1, j, NT_ + j))

                @pl.when(j < NT_ - 1)
                def _():
                    start(weights(1, j + 1, NT_ + j + 1))

                @pl.when(j == NT_ - 1)
                def _():
                    start(weights(0, 0, BOTH, True))

                projections(0, slot)
                projections(1, slot)
                back(0)
                apart(j > 0, lambda: sent(j - 1))
                apart((j > 2) & (j < 3 + EARLY), lambda: early_store(j - 3).wait())
                apart((j > 2) & (j < 2 + EARLY), lambda: early_send(j - 3).start())
                apart((j > 1) & (j < 2 + EARLY), lambda: early_begin(j - 2))
                da(lo, slot)
                back(1)
                da(hi, slot)
                apart(j == NT_ - 1, lambda: start([load_h(HB, 0), load_h(HB, 1), *loads(0)]))

                def gradients(i):
                    h = side_of(i)
                    for q in (0, 2):
                        put(2, h, dot(DT[q * R : (q + 2) * R, :], ACT[:, hidden_of(h)], NN), q)
                    for k, rhs in ((0, DG), (1, DU)):
                        put(k, h, dot(AT[half_of(h), :], rhs[:], NN))
                    apart(i == 0, lambda: send_far(j))

                loop(2, gradients)
                d2d(j, NEAR).start()
                keep(j).start()
                apart(j > 1, lambda: across(j - 2).wait_send())
                far_sum(j)
                across(j).start()
                apart((j > 1) & (j < 2 + EARLY), lambda: early_sum(j - 2))

            loop(NT_, tile)
            norm_back(HB)

        pl.run_scoped(layer1, pltpu.VMEM((2, D, CHUNK), BF16))

    first_half()

    def layer0():
        S = ((G0, U0, D0), (G1, U1, D1))

        def tile(j):
            t = NT_ + j
            slot = j % 2
            half_sum = pl.ds(0, W)

            def back(half):
                g_ref, u_ref, d_ref = S[half]
                product_back(lambda r, n: g_ref[r : r + n, :], lambda r, n: u_ref[r : r + n, :], d_ref, half * H)

            wait(weights(0, j, BOTH + j, True))

            @pl.when(j < NT_ - 1)
            def _():
                start(weights(0, j + 1, BOTH + j + 1, True))

            wait(loads(j))
            D0[:] = dot(DD[lo, :], WD[slot], NT).astype(BF16)
            D1[:] = dot(DD[hi, :], WD[slot], NT).astype(BF16)
            back(0)
            ACC[:, half_sum] = dot(DT[:, lo], ACT[lo, :], NN)
            back(1)
            apart(j < NT_ - 1, lambda: start(loads(j + 1)))
            apart(j == 0, lambda: load_a0t.wait())
            apart(j > 0, lambda: sent(t - 1))

            def gradients(i):
                h = side_of(i)
                for q in (0, 2):
                    rows = slice(q * R, (q + 2) * R)
                    put(2, h, ACC[rows, hidden_of(h)] + dot(DT[rows, hi], ACT[hi, hidden_of(h)], NN), q)
                for k, rhs in ((0, DG), (1, DU)):
                    put(k, h, dot(AT[half_of(h), :], rhs[:], NN))
                apart((j > 1) & (i == 0), lambda: (far_store(t - 1).wait(), across(t - 1, False).start()))
                apart(i == 0, lambda: send_far(t))

            loop(2, gradients)
            d2d(t, NEAR).start()
            keep(t).start()
            apart(j < 3, lambda: across(t - 2).wait_send())
            far_sum(t)
            apart(j == 0, lambda: across(t).start())
            apart(j > 0, lambda: far_store(t).start())

        loop(NT_, tile)

    layer0()

    last = BOTH - 1
    far_store(last).wait()
    across(last, False).start()
    early_send(EARLY - 1).start()
    sent(last)
    pl.semaphore_wait(free, 1)

    def finish():
        GN, UN, CB = GR.at[0, 1, 0], GR.at[0, 1, 1], GR.at[:, 0, 0]
        SQ[:] = jnp.zeros_like(SQ)

        def outs(t):
            l, j = 1 - t // NT_, t % NT_
            copies = []
            for p in range(DEVICES):
                copies.append(pltpu.make_async_copy(GN.at[:, pl.ds(p * LANES, LANES)], gg.at[l, :, columns(p, j)], fsem.at[3 + p]))
                copies.append(pltpu.make_async_copy(UN.at[:, pl.ds(p * LANES, LANES)], gu.at[l, :, columns(p, j)], fsem.at[7 + p]))
            rows = pl.ds(pl.multiple_of(j * LANES, LANES), LANES)
            copies.append(pltpu.make_async_copy(DN, gd.at[l, rows, :], fsem.at[11]))
            return copies

        def one(t):
            ins = [
                pltpu.make_async_copy(own.at[t], FB.at[0], fsem.at[0]),
                pltpu.make_async_copy(mate.at[t], FB.at[1], fsem.at[1]),
                pltpu.make_async_copy(cross.at[t], CB, fsem.at[2]),
            ]
            apart(t >= EARLY, lambda: d2d(t, NEAR).wait_recv())
            start(ins[:2])
            apart(t >= EARLY, lambda: across(t, False).wait_recv())
            ins[2].start()
            apart(t > NT_, lambda: across(t, False).wait_send())

            @pl.when(t > 0)
            def _():
                wait(outs(t - 1))

            wait(ins)
            for k in range(3):
                total = FB[0, k].astype(F32) + FB[1, k].astype(F32) + CB[k].astype(F32)
                g = total.astype(BF16)
                wide = g.astype(F32)
                SQ[:] += jnp.sum((wide * wide).reshape(R // 8, 8, W), axis=0)
                if k == 0:
                    GN[:] = g
                elif k == 1:
                    UN[:] = g
                else:
                    DN[:] = tall(g).T
            start(outs(t))

        loop(BOTH, one)

        mine = jnp.sum(SQ[:], keepdims=True)
        SQS[DEVICES] = jnp.broadcast_to(mine, (8, LANES))
        copies = [
            pltpu.make_async_remote_copy(
                src_ref=SQS.at[DEVICES], dst_ref=SQS.at[me], send_sem=sq_send.at[k - 1], recv_sem=sq_recv.at[k - 1],
                device_id={"dp": (me + k) % DEVICES}, device_id_type=pl.DeviceIdType.MESH)
            for k in range(1, DEVICES)
        ]
        start(copies)
        SQS[me] = jnp.broadcast_to(mine, (8, LANES))
        wait(outs(last))
        for k in range(1, DEVICES):
            came = SQS.at[(me + DEVICES - k) % DEVICES]
            pltpu.make_async_copy(came, came, sq_recv.at[k - 1]).wait()
            copies[k - 1].wait_send()

    finish()
    for c in moments():
        c.wait()
    for t in range(EARLY):
        early_send(t).wait()

    total = sum(SQS[k] for k in range(DEVICES))
    count = 2.0 * 3.0 * D * F
    factor[:] = jnp.minimum(1.0, 0.5 * lax.rsqrt(total / count + 1e-30))


def gradients(x, dy, wg, wu, wd, md, vd):
    T, D = x.shape
    F = wg.shape[2]
    W = DEVICES * LANES
    n, R = F // W, D // DEVICES
    tiles = 2 * n
    hbm = lambda *s, d=BF16: jax.ShapeDtypeStruct(s, d)
    outs = [
        hbm(2, R, F), hbm(2, R, F), hbm(2, F // DEVICES, D), hbm(8, LANES, d=F32),
        hbm(EARLY * LANES, D, d=F32), hbm(EARLY * LANES, D, d=F32), hbm(EARLY * LANES, D), hbm(EARLY * LANES, D),
        hbm(n, T, W, d=F32), hbm(n, T, W, d=F32), hbm(D, T), hbm(T // CHUNK, D, CHUNK),
        hbm(tiles, 3, R, W), hbm(tiles, 3, R, W), hbm(tiles, 3, R, W), hbm(tiles, 3, R, W),
    ]
    sem = pltpu.SemaphoreType.DMA
    return pl.pallas_call(
        grads_kernel,
        out_shape=outs,
        in_specs=[ANY] * 7,
        out_specs=[ANY] * 3 + [pl.BlockSpec(memory_space=pltpu.VMEM)] + [ANY] * 12,
        scratch_shapes=[
            pltpu.VMEM((LANES, D), BF16),
            pltpu.VMEM((T, D), BF16), pltpu.VMEM((D, T), BF16), pltpu.VMEM((T, D), BF16), pltpu.VMEM((D, T), BF16),
            pltpu.VMEM((D, T), F32), pltpu.VMEM((3, 2, 2, R, W), BF16), *[pltpu.VMEM((T, W), BF16)] * 3,
            pltpu.VMEM((2, D, W), BF16), pltpu.VMEM((2, D, W), BF16), pltpu.VMEM((2, W, D), BF16),
            *[pltpu.VMEM((T // 2, W), F32), pltpu.VMEM((T // 2, W), F32), pltpu.VMEM((T // 2, W), BF16)] * 2,
            pltpu.VMEM((3, R, W), BF16), pltpu.VMEM((2, 3, R, W), BF16),
            pltpu.VMEM((8, W), F32), pltpu.VMEM((DEVICES + 1, 8, LANES), F32),
            sem((2, 3, DEVICES)), sem((7,)), sem((2,)), sem(()), sem((tiles,)), pltpu.SemaphoreType.REGULAR, sem(()), sem(()),
            sem((tiles,)), sem((tiles,)), sem((12,)), sem((DEVICES - 1,)), sem((DEVICES - 1,)),
            sem((4,)), sem((2 + EARLY,)), sem((2 + EARLY,)),
        ],
        compiler_params=pltpu.CompilerParams(collective_id=0, has_side_effects=True, vmem_limit_bytes=VMEM_BYTES),
        name="gradients",
    )(x, dy, wg, wu, wd, md, vd)[:7]


def cost(n):
    return pl.CostEstimate(flops=4 * n, bytes_accessed=4 * n, transcendentals=0)


def stepped(factor, g, w, m, v):
    grad = g.astype(F32) * factor[:1, :1]
    m = 0.9 * m + 0.1 * grad
    v = 0.95 * v + 0.05 * grad * grad
    wide = w.astype(F32)
    return (wide - 0.02 * (m * lax.rsqrt(v + 1e-8) + 0.1 * wide)).astype(BF16), m, v


def adamw_kernel(me, factor, g, w, m, v, *refs):
    out, send, new_m, new_v, turn = refs[-5:]
    turn[0] = me[0]

    def part(i):
        r = pl.ds(pl.multiple_of(i * SOME, SOME), SOME)
        out[r, :], new_m[r, :], new_v[r, :] = stepped(factor, g[r, :], w[r, :], m[r, :], v[r, :])
        send[r, :] = out[r, :]

    loop(m.shape[0] // SOME, part)


def adamw(me, factor, g, w, m, v, so_far, layer, first, steps, by_columns):
    rows = m.shape[1] if by_columns else LANES
    cols = DEVICES * LANES if by_columns else m.shape[2]
    tile = (None, rows, cols)
    if by_columns:
        block = pl.BlockSpec(tile, lambda i, me: (layer, 0, first + i))
        whole = pl.BlockSpec(tile, lambda i, me: (layer, me[0], first + i))
        alone, send = (rows, steps * cols), pl.BlockSpec((rows, cols), lambda i, me: (0, i))
    else:
        n = m.shape[1] // LANES
        block = pl.BlockSpec(tile, lambda i, me: (layer, first + i, 0))
        whole = pl.BlockSpec(tile, lambda i, me: (layer, me[0] * n + first + i, 0))
        alone, send = (steps * rows, cols), pl.BlockSpec((rows, cols), lambda i, me: (i, 0))
    begun = so_far is not None
    shape = lambda a: jax.ShapeDtypeStruct(a.shape, a.dtype)
    out, sent, new_m, new_v, turn = pl.pallas_call(
        adamw_kernel,
        grid_spec=pltpu.PrefetchScalarGridSpec(
            num_scalar_prefetch=1,
            grid=(steps,),
            in_specs=[FACTOR, block, whole, block, block] + [ANY] * (3 * begun),
            out_specs=[whole, send, block, block, pl.BlockSpec(memory_space=pltpu.SMEM)],
        ),
        out_shape=[shape(w), jax.ShapeDtypeStruct(alone, BF16), shape(m), shape(v), shape(me)],
        input_output_aliases={6: 0, 7: 2, 8: 3} if begun else {},
        compiler_params=pltpu.CompilerParams(vmem_limit_bytes=VMEM_BYTES),
        cost_estimate=cost(5 * steps * rows * cols),
        name="adamw",
    )(me, factor, g, w, m, v, *(so_far or ()))
    return (out, new_m, new_v), sent, turn


def other_kernel(me, factor, g, w, m, v, _, out, send, turn):
    turn[0] = me[0]
    out[:], *_ = stepped(factor, g[:], w[:], m[:], v[:])
    send[:] = out[:]


def adamw_of_other(me, factor, g, w, m, v, out, layer):
    D = m.shape[1]
    n = w.shape[1] // DEVICES // LANES
    block = pl.BlockSpec((LANES, D), lambda i, me: (i, 0))
    whole = pl.BlockSpec((None, LANES, D), lambda i, me: (layer, (me[0] ^ 2) * n + i, 0))
    return pl.pallas_call(
        other_kernel,
        grid_spec=pltpu.PrefetchScalarGridSpec(
            num_scalar_prefetch=1,
            grid=(EARLY,),
            in_specs=[FACTOR, block, whole, block, block, ANY],
            out_specs=[whole, block, pl.BlockSpec(memory_space=pltpu.SMEM)],
        ),
        out_shape=[jax.ShapeDtypeStruct(w.shape, BF16), jax.ShapeDtypeStruct(m.shape, BF16), jax.ShapeDtypeStruct(me.shape, me.dtype)],
        input_output_aliases={6: 0},
        compiler_params=pltpu.CompilerParams(vmem_limit_bytes=VMEM_BYTES),
        cost_estimate=cost(m.size),
        name="adamw_of_other",
    )(me, factor, g, w, m, v, out)


def place_kernel(n, at, me_ref, _, *refs):
    pieces, out, turn, bufs, sems = refs[:n], refs[n], refs[n + 1], refs[n + 2 : 2 * n + 2], refs[2 * n + 2]
    turn[0] = me_ref[0]
    loads = [pltpu.make_async_copy(p, b, sems.at[0, k]) for k, (p, b) in enumerate(zip(pieces, bufs))]
    for c in loads:
        c.start()
    stores = []
    for k in range(n):
        loads[k].wait()
        stores.append(pltpu.make_async_copy(bufs[k], out.at[at(k, me_ref[0])], sems.at[1, k]))
        stores[k].start()
    for c in stores:
        c.wait()


def place(out, me, pieces, owners, layer, first, by_columns):
    rows, cols = pieces[0].shape

    def at(k, me):
        owner = me ^ owners[k]
        if by_columns:
            return layer, pl.ds(pl.multiple_of(owner * rows, 8), rows), pl.ds(first * DEVICES * LANES, cols)
        return layer, pl.ds(pl.multiple_of(owner * (out.shape[1] // DEVICES) + first * LANES, LANES), rows), slice(None)

    n = len(pieces)
    return pl.pallas_call(
        functools.partial(place_kernel, n, at),
        in_specs=[pl.BlockSpec(memory_space=pltpu.SMEM)] + [ANY] * (n + 1),
        out_specs=[ANY, pl.BlockSpec(memory_space=pltpu.SMEM)],
        out_shape=[jax.ShapeDtypeStruct(out.shape, out.dtype), jax.ShapeDtypeStruct(me.shape, me.dtype)],
        scratch_shapes=[pltpu.VMEM((rows, cols), BF16)] * n + [pltpu.SemaphoreType.DMA((2, n))],
        input_output_aliases={1: 0},
        compiler_params=pltpu.CompilerParams(vmem_limit_bytes=VMEM_BYTES),
        cost_estimate=cost(n * rows * cols),
        name="place",
    )(me, out, *pieces)


def other_chip(a):
    return lax.ppermute(a, "dp", [(i, i ^ 2) for i in range(4)])


def other_core(a):
    return lax.ppermute(a, "dp", [(i, i ^ 1) for i in range(4)])


ORDER = ((0, 0, (1, 2, 6)), (0, 1, (9,)), (1, 0, (9,)), (1, 1, (9,)), (2, 0, (9,)), (2, 1, (2, 2, 1)))


def chunks():
    listed = []
    for k, layer, sizes in ORDER:
        first = EARLY if (k, layer) == ORDER[-1][:2] else 0
        for n in sizes:
            listed.append((k, layer, first, n))
            first += n
    return listed


CHUNKS = chunks()


def solution(mesh):
    def step(x, dy, *arrays):
        weights, m, v = (arrays[i : i + 3] for i in (0, 3, 6))
        me = lax.axis_index("dp").astype(jnp.int32).reshape(1)
        *g, factor, m_other, v_other, g_other = gradients(x[0], dy[0], *weights, m[2], v[2])
        new = [None] * 3
        gathered = []
        for k, layer, first, steps in CHUNKS:
            new[k], sent, me = adamw(me, factor, g[k], weights[k], m[k], v[k], new[k], layer, first, steps, k < 2)
            far = other_chip(sent)
            own = other_core(sent)
            gathered.append((far, own, other_core(far)))
        new[2], sent, me = adamw(me, factor, g[2], weights[2], m[2], v[2], new[2], 1, 0, EARLY, False)
        whole = [n[0] for n in new]
        whole[2], far, me = adamw_of_other(me, factor, g_other, weights[2], m_other, v_other, whole[2], 1)
        own = other_core(sent)
        far = other_core(far)
        whole[2], me = place(whole[2], me, (own, far), (1, 3), 1, 0, False)
        for (k, layer, first, steps), pieces in zip(CHUNKS, gathered):
            whole[k], me = place(whole[k], me, pieces, (2, 1, 3), layer, first, k < 2)
        return (*whole, *(n[1] for n in new), *(n[2] for n in new))

    rows = P(None, "dp", None)
    return jax.shard_map(
        step,
        mesh=mesh,
        in_specs=(P(("rep", "dp")), P(("rep", "dp")), *(P(),) * 3, *(rows,) * 6),
        out_specs=(*(P("rep"),) * 3, *(P("rep", "dp"),) * 6),
        check_vma=False,
    )
```
